8 devices in a mesh: dp: 2 (over z, y), ep: 4 (over x, core).
Axes of the slice: x: 2, y: 2, z: 1, core: 2. Of those that a mesh axis runs over, the one named last changes fastest.
Arguments:
- x_norm: bfloat16 [2048, 4096], P(('dp', 'ep'))
- route_idx: int32 [2048, 4], P(('dp', 'ep'))
- w_router: bfloat16 [4096, 16], replicated
- w_gate: bfloat16 [16, 4096, 688], P('ep')
- w_up: bfloat16 [16, 4096, 688], P('ep')
- w_down: bfloat16 [16, 688, 4096], P('ep')
- grad_out: bfloat16 [2048, 4096], P(('dp', 'ep'))
Outputs:
- output 1: bfloat16 [2048, 4096], P(('dp', 'ep'))
- output 2: float32 [16, 4096, 688], P('ep')
- output 3: float32 [16, 4096, 688], P('ep')
- output 4: float32 [16, 688, 4096], P('ep')
- output 5: float32 [4096, 16], replicated
All inputs are finite; a program needn't handle non-finite values.
Results may differ from the reference program's by a relative error of at most 0.00549165.
Values are sent between devices in bfloat16 or wider.
A program may use at most 1 GiB of HBM per device.

```python
import jax
import jax.numpy as jnp
from jax import lax

D = 4096
FF = 688
EXPERTS = 16
TOP = 4
TOK_DEV = 256
SHARDS = 8
CAP = 192
TOKENS = SHARDS * TOK_DEV
N_CHOICE = TOKENS * TOP


def shuffle_rows(row_key):
    return jax.random.permutation(row_key, TOK_DEV)


def permute_rows(shard_rows, row_order):
    return shard_rows[row_order]


def draw_routes(route_key):
    perm_key, shift_key, order_key = jax.random.split(route_key, 3)
    expert_order = jax.random.permutation(perm_key, EXPERTS).astype(jnp.int32)
    shifts = jax.random.randint(shift_key, (SHARDS,), 0, EXPERTS - 1, dtype=jnp.int32)
    tok_pos = jnp.arange(TOK_DEV, dtype=jnp.int32)
    choice_pos = jnp.arange(TOP, dtype=jnp.int32)
    is_hot = tok_pos < CAP
    cycle_pos = (tok_pos * TOP - jnp.minimum(tok_pos, CAP))[:, None] + choice_pos[None, :] - is_hot[:, None].astype(jnp.int32)
    labels = 1 + (cycle_pos[None, :, :] + shifts[:, None, None]) % (EXPERTS - 1)
    hot_slot = is_hot[:, None] & (choice_pos[None, :] == 0)
    labels = jnp.where(hot_slot[None, :, :], 0, labels)
    experts = expert_order[labels]
    row_orders = jax.vmap(shuffle_rows)(jax.random.split(order_key, SHARDS))
    experts = jax.vmap(permute_rows)(experts, row_orders)
    return experts.reshape(TOKENS, TOP).astype(jnp.int32)


def setup_inputs(seed: int = 0) -> dict:
    base_key = jax.random.key(seed)
    key_list = jax.random.split(base_key, 7)
    x_norm = jax.random.normal(key_list[0], (TOKENS, D), jnp.float32)
    w_router = jax.random.normal(key_list[2], (D, EXPERTS), jnp.float32) * D ** -0.5
    w_gate = jax.random.normal(key_list[3], (EXPERTS, D, FF), jnp.float32) * D ** -0.5
    w_up = jax.random.normal(key_list[4], (EXPERTS, D, FF), jnp.float32) * D ** -0.5
    w_down = jax.random.normal(key_list[5], (EXPERTS, FF, D), jnp.float32) * FF ** -0.5
    grad_out = jax.random.normal(key_list[6], (TOKENS, D), jnp.float32)
    return {
        "x_norm": x_norm.astype(jnp.bfloat16),
        "route_idx": draw_routes(key_list[1]),
        "w_router": w_router.astype(jnp.bfloat16),
        "w_gate": w_gate.astype(jnp.bfloat16),
        "w_up": w_up.astype(jnp.bfloat16),
        "w_down": w_down.astype(jnp.bfloat16),
        "grad_out": grad_out.astype(jnp.bfloat16),
    }


def expert_backward(x_rows, dy_rows, gate_rows, w_gate_e, w_up_e, w_down_e):
    z_gate = jnp.dot(x_rows, w_gate_e, preferred_element_type=jnp.float32)
    z_up = jnp.dot(x_rows, w_up_e, preferred_element_type=jnp.float32)
    sigmoid_z = jax.nn.sigmoid(z_gate)
    silu_z = z_gate * sigmoid_z
    act_rows = (silu_z * z_up).astype(jnp.bfloat16)
    out_rows = jnp.dot(act_rows, w_down_e, preferred_element_type=jnp.float32)
    dy_wide = dy_rows.astype(jnp.float32)
    dgate_rows = jnp.sum(out_rows * dy_wide, axis=1)
    d_out = (gate_rows[:, None] * dy_wide).astype(jnp.bfloat16)
    d_act = jnp.dot(d_out, w_down_e.T, preferred_element_type=jnp.float32)
    d_zgate = (d_act * z_up * sigmoid_z * (1.0 + z_gate * (1.0 - sigmoid_z))).astype(jnp.bfloat16)
    d_zup = (d_act * silu_z).astype(jnp.bfloat16)
    dx_rows = (jnp.dot(d_zgate, w_gate_e.T, preferred_element_type=jnp.float32) + jnp.dot(d_zup, w_up_e.T, preferred_element_type=jnp.float32)).astype(jnp.bfloat16)
    grad_gate = jnp.dot(x_rows.T, d_zgate, preferred_element_type=jnp.float32)
    grad_up = jnp.dot(x_rows.T, d_zup, preferred_element_type=jnp.float32)
    grad_down = jnp.dot(act_rows.T, d_out, preferred_element_type=jnp.float32)
    return dx_rows, dgate_rows, grad_gate, grad_up, grad_down


def reference(x_norm, route_idx, w_router, w_gate, w_up, w_down, grad_out):
    logits = jnp.dot(x_norm, w_router, preferred_element_type=jnp.float32)
    gate_probs = jax.nn.softmax(jnp.take_along_axis(logits, route_idx, axis=1), axis=-1)
    expert_ids = jnp.arange(EXPERTS, dtype=jnp.int32)
    shard_idx = route_idx.reshape(SHARDS, TOK_DEV * TOP)
    one_hot = (shard_idx[:, :, None] == expert_ids).astype(jnp.int32)
    rank_in = jnp.sum((jnp.cumsum(one_hot, axis=1) - one_hot) * one_hot, axis=2)
    slot_ids = (shard_idx * (SHARDS * CAP) + jnp.arange(SHARDS, dtype=jnp.int32)[:, None] * CAP + rank_in).reshape(N_CHOICE)
    slot_table = jnp.full((EXPERTS * SHARDS * CAP,), N_CHOICE, jnp.int32).at[slot_ids].set(jnp.arange(N_CHOICE, dtype=jnp.int32)).reshape(EXPERTS, SHARDS * CAP)
    gate_flat = gate_probs.reshape(N_CHOICE)

    def one_expert(operands):
        w_gate_e, w_up_e, w_down_e, choice_ids = operands
        is_valid = choice_ids < N_CHOICE
        safe_ids = jnp.minimum(choice_ids, N_CHOICE - 1)
        x_rows = jnp.where(is_valid[:, None], x_norm[safe_ids // TOP], 0.0)
        dy_rows = jnp.where(is_valid[:, None], grad_out[safe_ids // TOP], 0.0)
        gate_rows = jnp.where(is_valid, gate_flat[safe_ids], 0.0)
        return expert_backward(x_rows, dy_rows, gate_rows, w_gate_e, w_up_e, w_down_e)

    dx_rows, dgate_rows, grad_gate, grad_up, grad_down = lax.map(one_expert, (w_gate, w_up, w_down, slot_table))
    dx_choice = dx_rows.reshape(EXPERTS * SHARDS * CAP, D)[slot_ids].reshape(TOKENS, TOP, D)
    dgate = dgate_rows.reshape(EXPERTS * SHARDS * CAP)[slot_ids].reshape(TOKENS, TOP)
    d_sel = gate_probs * (dgate - jnp.sum(gate_probs * dgate, axis=1, keepdims=True))
    d_logits = jnp.sum(jnp.where(route_idx[:, :, None] == expert_ids, d_sel[:, :, None], 0.0), axis=1).astype(jnp.bfloat16)
    du_router = jnp.dot(d_logits, w_router.T, preferred_element_type=jnp.float32)
    grad_x = (jnp.sum(dx_choice.astype(jnp.float32), axis=1) + du_router).astype(jnp.bfloat16)
    grad_router = jnp.dot(x_norm.T, d_logits, preferred_element_type=jnp.float32)
    return grad_x, grad_gate, grad_up, grad_down, grad_router
```

```python
import functools

import jax
import jax.numpy as jnp
from jax import lax
from jax.experimental import pallas as pl
from jax.experimental.pallas import tpu as pltpu
from jax.sharding import PartitionSpec as P


COLD = 64
OVER = 128
VMEM_LIMIT = 62 * 1024 * 1024
F32 = jnp.float32
BF16 = jnp.bfloat16

NN = (((1,), (0,)), ((), ()))
NT = (((1,), (1,)), ((), ()))
TN = (((0,), (0,)), ((), ()))


def mm(a, b, dims):
    return lax.dot_general(a, b, dims, preferred_element_type=F32)


def tile_of(step):
    return jnp.where(step < 4, step, 4 + (step - 4) // 2)


def cost(flops, nbytes):
    return pl.CostEstimate(flops=int(flops), bytes_accessed=int(nbytes), transcendentals=0)


def dispatch_kernel(with_g, info, *refs):
    xs, gs, metas = refs[0:4], refs[4:8], refs[8:12]
    x_out, do_out = refs[12], refs[13]
    g_out = refs[14] if with_g else None
    step = pl.program_id(1)

    def piece(k, expert, n_rows, base, lo):
        rank = metas[k][pl.ds(expert, 1), :]
        gate = metas[k][pl.ds(16 + expert, 1), :]
        row = lax.broadcasted_iota(jnp.int32, (n_rows, rank.shape[1]), 0).astype(F32) + float(base)
        hit = rank == row
        sel = jnp.where(hit, 1.0, 0.0).astype(BF16)
        gate_col = jnp.sum(jnp.where(hit, gate, 0.0), axis=1, keepdims=True)
        x_out[0, lo:lo + n_rows, :] = mm(sel, xs[k][...], NN).astype(BF16)
        g_rows = mm(sel, gs[k][...], NN)
        do_out[0, lo:lo + n_rows, :] = (gate_col * g_rows).astype(BF16)
        if with_g:
            g_out[0, lo:lo + n_rows, :] = g_rows.astype(BF16)

    @pl.when(step < 4)
    def _():
        for k in range(4):
            piece(k, info[0] + step, COLD, 0, COLD * k)

    for q in range(2):
        @pl.when(step == 4 + q)
        def _():
            for half in range(2):
                k = 2 * q + half
                piece(k, info[0] + info[1 + k], OVER, COLD, OVER * half)


def dispatch(info, xs, gs, metas, with_g):
    tok, dim = xs[0].shape
    dc = 1024
    blk = pl.BlockSpec((tok, dc), lambda c, i, s: (0, c))
    meta_blk = pl.BlockSpec(metas[0].shape, lambda c, i, s: (0, 0))
    out_blk = pl.BlockSpec((1, 256, dc), lambda c, i, s: (i, 0, c))
    n_out = 3 if with_g else 2
    return pl.pallas_call(
        functools.partial(dispatch_kernel, with_g),
        grid_spec=pltpu.PrefetchScalarGridSpec(
            num_scalar_prefetch=1, grid=(dim // dc, 6),
            in_specs=[blk] * 8 + [meta_blk] * 4, out_specs=[out_blk] * n_out),
        out_shape=[jax.ShapeDtypeStruct((6, 256, dim), BF16)] * n_out,
        compiler_params=pltpu.CompilerParams(vmem_limit_bytes=VMEM_LIMIT),
        cost_estimate=cost(2 * 2 * 1536 * 256 * dim, 2 * 3 * 1536 * dim * 2),
        name="dispatch",
    )(info, *xs, *gs, *metas)


def hidden_kernel(with_g, n_c, eidx, act, *refs):
    if with_g:
        x, do, g, w1, w3, w2, a_out, d1_out, d3_out, q_out, d1r_out, d3r_out, z1, z3, da, hg = refs
    else:
        x, do, w1, w3, w2, a_out, d1_out, d3_out, z1, z3, da = refs
    step, c = pl.program_id(0), pl.program_id(1)

    def terms():
        out = [(z1, mm(w1[0], x[0], NT)), (z3, mm(w3[0], x[0], NT)), (da, mm(w2[0], do[0], NT))]
        if with_g:
            out.append((hg, mm(w2[0], g[0], NT)))
        return out

    @pl.when((act[step] == 1) & (c == 0))
    def _():
        for ref, val in terms():
            ref[...] = val

    @pl.when((act[step] == 1) & (c > 0))
    def _():
        for ref, val in terms():
            ref[...] += val

    def finish(lo):
        n = 128
        z_gate, z_up, d_act = z1[:, lo:lo + n], z3[:, lo:lo + n], da[:, lo:lo + n]
        sig = jax.nn.sigmoid(z_gate)
        silu = z_gate * sig
        a = (silu * z_up).astype(BF16)
        d1 = (d_act * z_up * sig * (1.0 + z_gate * (1.0 - sig))).astype(BF16)
        d3 = (d_act * silu).astype(BF16)
        a_out[0, :, lo:lo + n] = a
        d1_out[0, :, lo:lo + n] = d1
        d3_out[0, :, lo:lo + n] = d3
        if with_g:
            q = jnp.sum(a.astype(F32) * hg[:, lo:lo + n], axis=0, keepdims=True)
            q_out[0, :, lo:lo + n] = jnp.broadcast_to(q, (8, n))
            d1r_out[0, lo:lo + n, :] = d1.astype(F32).T.astype(BF16)
            d3r_out[0, lo:lo + n, :] = d3.astype(F32).T.astype(BF16)

    @pl.when((act[step] == 1) & (c == n_c - 1))
    def _():
        @pl.when((step != 5) & (step != 7))
        def _():
            finish(0)

        finish(128)


def hidden(eidx, act, rows, w1t, w3t, w2):
    with_g = len(rows) == 3
    ff, dim = w1t.shape[1:]
    dc = 1024
    n_c = dim // dc

    def cc(i, c, act):
        return jnp.where(act[i] == 1, c, n_c - 1)

    row_blk = pl.BlockSpec((1, 256, dc), lambda i, c, e, t: (tile_of(i), 0, cc(i, c, t)))
    w_blk = pl.BlockSpec((1, ff, dc), lambda i, c, e, t: (e[i], 0, cc(i, c, t)))

    def out(d0, d1, dtype):
        return (jax.ShapeDtypeStruct((6, d0, d1), dtype),
                pl.BlockSpec((1, d0, d1), lambda i, c, e, t: (tile_of(i), 0, 0)))

    outs = [out(ff, 256, BF16)] * 3
    if with_g:
        outs += [out(8, 256, F32), out(256, ff, BF16), out(256, ff, BF16)]
    n_mm = 4 if with_g else 3
    return pl.pallas_call(
        functools.partial(hidden_kernel, with_g, n_c),
        grid_spec=pltpu.PrefetchScalarGridSpec(
            num_scalar_prefetch=2, grid=(8, n_c),
            in_specs=[row_blk] * len(rows) + [w_blk] * 3, out_specs=[o[1] for o in outs],
            scratch_shapes=[pltpu.VMEM((ff, 256), F32)] * n_mm),
        out_shape=[o[0] for o in outs],
        compiler_params=pltpu.CompilerParams(vmem_limit_bytes=VMEM_LIMIT),
        cost_estimate=cost(n_mm * 2 * 1536 * dim * ff, 100e6),
        name="hidden",
    )(eidx, act, *rows, w1t, w3t, w2)


def back_kernel(eidx, act, d1, d3, w1, w3, s0, s1, s2, s3, o0, o1, o2, o3, r_sc):
    step = pl.program_id(1)
    slots, outs = (s0, s1, s2, s3), (o0, o1, o2, o3)

    @pl.when(act[step] == 1)
    def _():
        r = (mm(d1[0], w1[0], NN) + mm(d3[0], w3[0], NN)).astype(BF16)

        @pl.when(step < 4)
        def _():
            for k in range(4):
                r_sc[k, pl.ds(pl.multiple_of(step * COLD, COLD), COLD), :] = r[COLD * k:COLD * (k + 1)]

        for q in range(2):
            @pl.when(step == 4 + 2 * q)
            def _():
                r_sc[2 * q, 256:384, :] = r[0:128]

            @pl.when((step == 4 + 2 * q) | (step == 5 + 2 * q))
            def _():
                r_sc[2 * q + 1, 256:384, :] = r[128:256]

    @pl.when(step == 7)
    def _():
        lane = lax.broadcasted_iota(jnp.int32, (256, 384), 1).astype(F32)
        for k in range(4):
            hit = lane == slots[k][:, 0:1]
            for m in range(1, 5):
                hit = hit | (lane == slots[k][:, m:m + 1])
            sel = jnp.where(hit, 1.0, 0.0).astype(BF16)
            outs[k][...] = mm(sel, r_sc[k], NN)


def back(eidx, act, d1, d3, w1t, w3t, slots):
    ff, dim = w1t.shape[1:]
    dc = 1024

    d_blk = pl.BlockSpec((1, 256, ff), lambda c, i, e, t: (tile_of(i), 0, 0))
    w_blk = pl.BlockSpec((1, ff, dc), lambda c, i, e, t: (e[i], 0, c))
    s_blk = pl.BlockSpec((256, 8), lambda c, i, e, t: (0, 0))
    o_blk = pl.BlockSpec((256, dc), lambda c, i, e, t: (0, c))
    return pl.pallas_call(
        back_kernel,
        grid_spec=pltpu.PrefetchScalarGridSpec(
            num_scalar_prefetch=2, grid=(dim // dc, 8),
            in_specs=[d_blk, d_blk, w_blk, w_blk] + [s_blk] * 4, out_specs=[o_blk] * 4,
            scratch_shapes=[pltpu.VMEM((4, 384, dc), BF16)]),
        out_shape=[jax.ShapeDtypeStruct((256, dim), F32)] * 4,
        compiler_params=pltpu.CompilerParams(vmem_limit_bytes=VMEM_LIMIT),
        cost_estimate=cost(2 * 2 * 1536 * dim * ff, 70e6),
        name="back",
    )(eidx, act, d1, d3, w1t, w3t, *slots)


def wgrad_kernel(info, xa, xb, ga, gb, xoa, xob, goa, gob,
                 aa, d1a, d3a, ab, d1b, d3b, w1o, w3o, w2o):
    j = pl.program_id(1)
    all_hot = info[1] == j
    for m in range(2, 9):
        all_hot = all_hot & (info[m] == j)

    def run(first, second):
        def main(n):
            x, g, _, _, a, d1, d3, _ = n
            return [(x[0], g[0], a[j], d1[j], d3[j])]

        def over(n):
            _, _, xo, go, a, d1, d3, _ = n
            return [(xo[q], go[q], a[4 + q], d1[4 + q], d3[4 + q]) for q in range(2)]

        def products(parts):
            w1o[0] = sum(mm(p[3], p[0], NN) for p in parts)
            w3o[0] = sum(mm(p[4], p[0], NN) for p in parts)
            w2o[0] = sum(mm(p[2], p[1], NN) for p in parts)

        @pl.when(all_hot)
        def _():
            products(main(first) + main(second) + over(first) + over(second))

        @pl.when(jnp.logical_not(all_hot))
        def _():
            products(main(first) + main(second))
            for n in (first, second):
                _, _, xo, go, a, d1, d3, off = n

                def body(q, _):
                    h0, h1 = info[off + 2 * q], info[off + 2 * q + 1]

                    @pl.when((h0 == j) | (h1 == j))
                    def _():
                        row = lax.broadcasted_iota(jnp.int32, (d1.shape[1], 256), 1)
                        mine = jnp.where(row < 128, h0, h1) == j

                        def keep(v):
                            return jnp.where(mine, v.astype(F32), 0.0).astype(BF16)

                        xq, gq = xo[q], go[q]
                        w1o[0] += mm(keep(d1[4 + q]), xq, NN)
                        w3o[0] += mm(keep(d3[4 + q]), xq, NN)
                        w2o[0] += mm(keep(a[4 + q]), gq, NN)

                    return 0

                lax.fori_loop(0, 2, body, 0)

    na = (xa, ga, xoa, goa, aa, d1a, d3a, 1)
    nb = (xb, gb, xob, gob, ab, d1b, d3b, 5)

    @pl.when(info[0] == 0)
    def _():
        run(na, nb)

    @pl.when(info[0] == 1)
    def _():
        run(nb, na)


def wgrad(info, xa, ga, hid_a, xb, gb, hid_b, dim, ff):
    dc = 512
    main_blk = pl.BlockSpec((1, 256, dc), lambda c, j, s: (j, 0, c))
    over_blk = pl.BlockSpec((2, 256, dc), lambda c, j, s: (2, 0, c))
    full_blk = pl.BlockSpec((6, ff, 256), lambda c, j, s: (0, 0, 0))
    return pl.pallas_call(
        wgrad_kernel,
        grid_spec=pltpu.PrefetchScalarGridSpec(
            num_scalar_prefetch=1, grid=(dim // dc, 4),
            in_specs=[main_blk] * 4 + [over_blk] * 4 + [full_blk] * 6,
            out_specs=[pl.BlockSpec((1, ff, dc), lambda c, j, s: (j, 0, c))] * 3),
        out_shape=[jax.ShapeDtypeStruct((4, ff, dim), F32)] * 3,
        compiler_params=pltpu.CompilerParams(vmem_limit_bytes=VMEM_LIMIT),
        cost_estimate=cost(3 * 2 * 3072 * dim * ff, 200e6),
        name="wgrad",
    )(info, xa, xb, ga, gb, xa, xb, ga, gb, *hid_a, *hid_b)


def solution(mesh):
    tok_spec = P(("dp", "ep"), None)
    exp_spec = P("ep", None, None)
    axes = ("dp", "ep")

    def shift(arr, dp_bit, ep_bits):
        pairs = [(s, (((s // 4) ^ dp_bit) * 4) + ((s % 4) ^ ep_bits)) for s in range(8)]
        return lax.ppermute(arr, axes, pairs)

    def device_step(x_loc, route_idx, w_router, w_gate, w_up, w_down, dy_loc):
        tok, dim = x_loc.shape
        ff = w_gate.shape[2]
        ep = lax.axis_index("ep")
        dp = lax.axis_index("dp")
        e0 = ep * 4
        w1t, w3t, w2 = jnp.swapaxes(w_gate, 1, 2), jnp.swapaxes(w_up, 1, 2), w_down

        logits = jnp.dot(x_loc, w_router, preferred_element_type=F32)
        hit = route_idx[:, :, None] == jnp.arange(16, dtype=jnp.int32)
        chosen = jnp.sum(jnp.where(hit, logits[:, None, :], 0.0), axis=2)
        probs = jax.nn.softmax(chosen, axis=-1)
        gate16 = jnp.sum(jnp.where(hit, probs[:, :, None], 0.0), axis=1)
        picked = jnp.any(hit, axis=1)
        order = jnp.arange(tok, dtype=jnp.int32)
        before = (order[:, None] > order[None, :]).astype(BF16)
        rank16 = jnp.dot(before, picked.astype(BF16), preferred_element_type=F32)
        rank16 = jnp.where(picked, rank16, -1.0)
        meta = jnp.concatenate([rank16, gate16], axis=1).T

        def fan(block, dp_bit, ep_bits):
            return tuple(shift(v, dp_bit, ep_bits) for v in block)

        own = (x_loc, dy_loc, meta)
        across = fan(own, 0, 2)
        sib = fan(own, 0, 1)
        y_own = fan(own, 1, 0)
        across_sib = fan(across, 0, 1)
        y_across = fan(across, 1, 0)
        y_sib = fan(y_own, 0, 1)
        group_a = (own, sib, across, across_sib)

        def tables(group):
            ranks = jnp.stack([lax.dynamic_slice_in_dim(b[2], e0, 4, axis=0) for b in group])
            large = jnp.max(ranks, axis=2) >= COLD
            hot = jnp.where(jnp.any(large, axis=1), jnp.argmax(large, axis=1), 3).astype(jnp.int32)
            one = jnp.ones((), jnp.int32)
            eidx = jnp.concatenate([jnp.arange(4, dtype=jnp.int32), hot])
            act = jnp.stack([one, one, one, one, one, (hot[0] != hot[1]).astype(jnp.int32),
                             one, (hot[2] != hot[3]).astype(jnp.int32)])
            info = jnp.concatenate([e0[None].astype(jnp.int32), hot])
            return ranks, hot, eidx, act, info

        ranks_a, hot_a, eidx_a, act_a, info_a = tables(group_a)
        xa, da, ga = dispatch(info_a, [b[0] for b in group_a], [b[1] for b in group_a], [b[2] for b in group_a], True)
        a_a, d1_a, d3_a, q_a, d1r_a, d3r_a = hidden(eidx_a, act_a, (xa, da, ga), w1t, w3t, w2)

        local = jnp.arange(4, dtype=F32)[None, :, None]
        main_slot = jnp.where((ranks_a >= 0) & (ranks_a < COLD), ranks_a + COLD * local, -1.0)
        over_slot = jnp.max(jnp.where(ranks_a >= COLD, ranks_a - COLD + 4 * COLD, -1.0), axis=1, keepdims=True)
        slots = jnp.concatenate([main_slot, over_slot, jnp.full((4, 3, tok), -1.0, F32)], axis=1)
        slots = jnp.swapaxes(slots, 1, 2)
        part = back(eidx_a, act_a, d1r_a, d3r_a, w1t, w3t, [slots[k] for k in range(4)])

        q_rows = q_a[:, 0, :]
        q_main = q_rows[:4].reshape(4, 4, COLD).transpose(1, 0, 2)
        q_over = q_rows[4:].reshape(4, OVER)
        r64 = jnp.arange(COLD, dtype=F32)
        r128 = jnp.arange(OVER, dtype=F32) + COLD
        q_tok = jnp.sum(jnp.where(ranks_a[..., None] == r64, q_main[:, :, None, :], 0.0), axis=3)
        q_tok = q_tok + jnp.sum(jnp.where(ranks_a[..., None] == r128, q_over[:, None, None, :], 0.0), axis=3)
        q_back = jnp.stack([q_tok[0]] + [shift(q_tok[k], 0, k) for k in (1, 2, 3)])
        q16 = q_back[ep ^ jnp.arange(4, dtype=jnp.int32)].reshape(16, tok)

        gate_t = meta[16:]
        d_sel = gate_t * (q16 - jnp.sum(gate_t * q16, axis=0, keepdims=True))
        d_logits = d_sel.astype(BF16)
        du = lax.dot_general(d_logits, w_router, (((0,), (1,)), ((), ())), preferred_element_type=F32)
        gr = jnp.dot(d_logits, x_loc, preferred_element_type=F32)
        gr = gr + shift(gr, 0, 1)
        gr = gr + shift(gr, 0, 2)
        grad_router = (gr + shift(gr, 1, 0)).T

        part_own, y_own, y_sib, y_across = lax.optimization_barrier((part[0], y_own, y_sib, y_across))
        y_across_sib = fan(y_across, 0, 1)
        group_b = (y_own, y_sib, y_across, y_across_sib)
        _, hot_b, eidx_b, act_b, info_b = tables(group_b)
        xb, db = dispatch(info_b, [b[0] for b in group_b], [b[1] for b in group_b], [b[2] for b in group_b], False)

        to_sib = shift(part[1], 0, 1)
        pair = part[2] + shift(part[3], 0, 1)
        xb, db, pair = lax.optimization_barrier((xb, db, pair))
        from_across = shift(pair, 0, 2)

        a_b, d1_b, d3_b = hidden(eidx_b, act_b, (xb, db), w1t, w3t, w2)
        info = jnp.concatenate([dp[None].astype(jnp.int32), hot_a, hot_b])
        g1t, g3t, grad_down = wgrad(info, xa, da, (a_a, d1_a, d3_a), xb, db, (a_b, d1_b, d3_b), dim, ff)
        grad_gate, grad_up = jnp.swapaxes(g1t, 1, 2), jnp.swapaxes(g3t, 1, 2)
        grad_x = (part_own + to_sib + from_across + du).astype(BF16)
        return grad_x, grad_gate, grad_up, grad_down, grad_router

    return jax.shard_map(device_step, mesh=mesh, in_specs=(tok_spec, tok_spec, P(), exp_spec, exp_spec, exp_spec, tok_spec), out_specs=(tok_spec, exp_spec, exp_spec, exp_spec, P()), check_vma=False)
```

```python
import functools

import jax
import jax.numpy as jnp
from jax import lax
from jax.experimental import pallas as pl
from jax.experimental.pallas import tpu as pltpu
from jax.sharding import PartitionSpec as P


COLD = 64
OVER = 128
VMEM_LIMIT = 62 * 1024 * 1024
F32 = jnp.float32
BF16 = jnp.bfloat16

NN = (((1,), (0,)), ((), ()))
NT = (((1,), (1,)), ((), ()))


def mm(a, b, dims):
    return lax.dot_general(a, b, dims, preferred_element_type=F32)


def tile_of(step, eidx):
    return jnp.where(step < 4, eidx[step], 4 + (step - 4) // 2)


def cost(flops, nbytes):
    return pl.CostEstimate(flops=int(flops), bytes_accessed=int(nbytes), transcendentals=0)


def dispatch_kernel(with_g, gated, slots, *refs):
    if gated:
        gates, v, refs = refs[0], refs[1:5], refs[5:]
        do_out, g_out = refs[0], (refs[1] if with_g else None)
        sel, col = refs[-2:]
    else:
        v, (x_out, sel) = refs[0:4], refs[4:]

    @pl.when(pl.program_id(0) == 0)
    def _():
        for k in range(4):
            for m in range(5):
                n = OVER if m == 4 else COLD
                lo = COLD * m
                row = lax.broadcasted_iota(jnp.int32, (n, 256), 0).astype(F32) + float(lo)
                hit = slots[k, m:m + 1, :] == row
                sel[k, lo:lo + n, :] = jnp.where(hit, 1.0, 0.0).astype(BF16)
                if gated:
                    col[k, lo:lo + n, :] = jnp.sum(jnp.where(hit, gates[k, m:m + 1, :], 0.0), axis=1, keepdims=True)

    def put(out, k, rows):
        for j in range(4):
            out[j, COLD * k:COLD * (k + 1), :] = rows[COLD * j:COLD * (j + 1)]
        out[4 + k // 2, OVER * (k % 2):OVER * (k % 2) + OVER, :] = rows[256:384]

    for k in range(4):
        rows = mm(sel[k], v[k][...], NN)
        if gated:
            put(do_out, k, (col[k] * rows).astype(BF16))
            if with_g:
                put(g_out, k, rows.astype(BF16))
        else:
            put(x_out, k, rows.astype(BF16))


def dispatch(slots, gates, vs, with_g):
    tok, dim = vs[0].shape
    dc = 512
    gated = gates is not None
    small = pl.BlockSpec((4, 8, 256), lambda c: (0, 0, 0))
    n_out = 2 if with_g else 1
    scratch = [pltpu.VMEM((4, 384, 256), BF16)]
    if gated:
        scratch.append(pltpu.VMEM((4, 384, 1), F32))
    return pl.pallas_call(
        functools.partial(dispatch_kernel, with_g, gated),
        grid=(dim // dc,),
        in_specs=[small] * (2 if gated else 1) + [pl.BlockSpec((tok, dc), lambda c: (0, c))] * 4,
        out_specs=[pl.BlockSpec((6, 256, dc), lambda c: (0, 0, c))] * n_out,
        out_shape=[jax.ShapeDtypeStruct((6, 256, dim), BF16)] * n_out,
        scratch_shapes=scratch,
        compiler_params=pltpu.CompilerParams(vmem_limit_bytes=VMEM_LIMIT),
        cost_estimate=cost(2 * 1536 * 256 * dim, 2 * n_out * 1536 * dim * 2),
        name="dispatch",
    )(*([slots, gates] if gated else [slots]), *vs)


def tile_kernel_call(kernel, eidx, act, rows, weights, late, outs, n_mm):
    ff, dim = weights[0].shape[1:]
    dc = 2048
    n_c = dim // dc

    def last(c, i, e):
        return jnp.where(c == n_c - 1, tile_of(i, e), tile_of(0, e))

    row_blk = pl.BlockSpec((1, 256, dc), lambda c, i, e, t: (tile_of(i, e), 0, c))
    w_blk = pl.BlockSpec((1, ff, dc), lambda c, i, e, t: (e[i], 0, c))
    late_blk = pl.BlockSpec((1, ff, 256), lambda c, i, e, t: (last(c, i, e), 0, 0))
    return pl.pallas_call(
        functools.partial(kernel, n_c),
        grid_spec=pltpu.PrefetchScalarGridSpec(
            num_scalar_prefetch=2, grid=(n_c, 8),
            in_specs=[row_blk] * len(rows) + [w_blk] * len(weights) + [late_blk] * len(late),
            out_specs=[pl.BlockSpec((1,) + o.shape[1:], lambda c, i, e, t: (last(c, i, e), 0, 0)) for o in outs],
            scratch_shapes=[pltpu.VMEM((8, ff, 256), F32)] * n_mm),
        out_shape=outs,
        compiler_params=pltpu.CompilerParams(vmem_limit_bytes=VMEM_LIMIT),
        cost_estimate=cost(n_mm * 2 * 1536 * dim * ff, 80e6),
    )(eidx, act, *rows, *weights, *late)


def accumulate(act, acc, terms, n_c, finish):
    c, step = pl.program_id(0), pl.program_id(1)

    @pl.when(act[step] == 1)
    def _():
        for ref, val in zip(acc, terms()):
            ref[step] = jnp.where(c == 0, 0.0, ref[step]) + val

    @pl.when((act[step] == 1) & (c == n_c - 1))
    def _():
        @pl.when((step != 5) & (step != 7))
        def _():
            finish(step, 0)

        finish(step, 128)


def forward_kernel(n_c, eidx, act, x, w1, w3, s_out, zu_out, sp_out, a_out, z1, z3):
    def terms():
        yield mm(w1[0], x[0], NT)
        yield mm(w3[0], x[0], NT)

    def finish(step, lo):
        n = 128
        z_gate, z_up = z1[step, :, lo:lo + n], z3[step, :, lo:lo + n]
        sig = jax.nn.sigmoid(z_gate)
        silu = z_gate * sig
        s_out[0, :, lo:lo + n] = silu
        zu_out[0, :, lo:lo + n] = z_up
        sp_out[0, :, lo:lo + n] = sig * (1.0 + z_gate * (1.0 - sig))
        a_out[0, :, lo:lo + n] = (silu * z_up).astype(BF16)

    accumulate(act, (z1, z3), terms, n_c, finish)


def hidden_grad_kernel(with_g, n_c, eidx, act, *refs):
    if with_g:
        do, g, w2, s_in, zu_in, sp_in, a_in, d1_out, d3_out, q_out, d1r_out, d3r_out, da, hg = refs
    else:
        do, w2, s_in, zu_in, sp_in, d1_out, d3_out, da = refs

    def terms():
        yield mm(w2[0], do[0], NT)
        if with_g:
            yield mm(w2[0], g[0], NT)

    def finish(step, lo):
        n = 128
        d_act = da[step, :, lo:lo + n]
        d1 = (d_act * zu_in[0, :, lo:lo + n] * sp_in[0, :, lo:lo + n]).astype(BF16)
        d3 = (d_act * s_in[0, :, lo:lo + n]).astype(BF16)
        d1_out[0, :, lo:lo + n] = d1
        d3_out[0, :, lo:lo + n] = d3
        if with_g:
            a = a_in[0, :, lo:lo + n].astype(F32)
            q = jnp.sum(a * hg[step, :, lo:lo + n], axis=0, keepdims=True)
            q_out[0, :, lo:lo + n] = jnp.broadcast_to(q, (8, n))
            d1r_out[0, lo:lo + n, :] = d1.astype(F32).T.astype(BF16)
            d3r_out[0, lo:lo + n, :] = d3.astype(F32).T.astype(BF16)

    accumulate(act, (da, hg) if with_g else (da,), terms, n_c, finish)


def forward(eidx, act, x, w1t, w3t):
    ff = w1t.shape[1]
    outs = [jax.ShapeDtypeStruct((6, ff, 256), F32)] * 3 + [jax.ShapeDtypeStruct((6, ff, 256), BF16)]
    return tile_kernel_call(forward_kernel, eidx, act, [x], [w1t, w3t], [], outs, 2)


def hidden_grad(eidx, act, rows, w2, late):
    ff = w2.shape[1]
    with_g = len(rows) == 2
    outs = [jax.ShapeDtypeStruct((6, ff, 256), BF16)] * 2
    if with_g:
        outs += [jax.ShapeDtypeStruct((6, 8, 256), F32)] + [jax.ShapeDtypeStruct((6, 256, ff), BF16)] * 2
    kernel = functools.partial(hidden_grad_kernel, with_g)
    return tile_kernel_call(kernel, eidx, act, rows, [w2], late, outs, len(rows))


def back_kernel(eidx, act, d1, d3, w1, w3, s0, s1, s2, s3, o0, o1, o2, o3, r_sc):
    step = pl.program_id(1)
    slots, outs = (s0, s1, s2, s3), (o0, o1, o2, o3)

    def rows(cols):
        r = (mm(d1[0], w1[0, :, cols], NN) + mm(d3[0], w3[0, :, cols], NN)).astype(BF16)

        @pl.when(step < 4)
        def _():
            lo = pl.multiple_of(eidx[step] * COLD, COLD)
            for k in range(4):
                r_sc[k, pl.ds(lo, COLD), cols] = r[COLD * k:COLD * (k + 1)]

        for q in range(2):
            @pl.when(step == 4 + 2 * q)
            def _():
                r_sc[2 * q, 256:384, cols] = r[0:128]

            @pl.when((step == 4 + 2 * q) | (step == 5 + 2 * q))
            def _():
                r_sc[2 * q + 1, 256:384, cols] = r[128:256]

    @pl.when(act[step] == 1)
    def _():
        def body(h, _):
            rows(pl.ds(pl.multiple_of(h * 1024, 1024), 1024))
            return 0

        lax.fori_loop(0, w1.shape[2] // 1024, body, 0)

    @pl.when(step == 7)
    def _():
        lane = lax.broadcasted_iota(jnp.int32, (256, 384), 1).astype(F32)
        for k in range(4):
            hit = lane == slots[k][:, 0:1]
            for m in range(1, 5):
                hit = hit | (lane == slots[k][:, m:m + 1])
            sel = jnp.where(hit, 1.0, 0.0).astype(BF16)
            outs[k][...] = mm(sel, r_sc[k], NN)


def back(eidx, act, d1, d3, w1t, w3t, slots):
    ff, dim = w1t.shape[1:]
    dc = 2048

    d_blk = pl.BlockSpec((1, 256, ff), lambda c, i, e, t: (tile_of(i, e), 0, 0))
    w_blk = pl.BlockSpec((1, ff, dc), lambda c, i, e, t: (e[i], 0, c))
    s_blk = pl.BlockSpec((256, 8), lambda c, i, e, t: (0, 0))
    o_blk = pl.BlockSpec((256, dc), lambda c, i, e, t: (0, c))
    return pl.pallas_call(
        back_kernel,
        grid_spec=pltpu.PrefetchScalarGridSpec(
            num_scalar_prefetch=2, grid=(dim // dc, 8),
            in_specs=[d_blk, d_blk, w_blk, w_blk] + [s_blk] * 4, out_specs=[o_blk] * 4,
            scratch_shapes=[pltpu.VMEM((4, 384, dc), BF16)]),
        out_shape=[jax.ShapeDtypeStruct((256, dim), F32)] * 4,
        compiler_params=pltpu.CompilerParams(vmem_limit_bytes=VMEM_LIMIT),
        cost_estimate=cost(2 * 2 * 1536 * dim * ff, 70e6),
        name="back",
    )(eidx, act, d1, d3, w1t, w3t, *slots)


def wgrad_kernel(info, xa, xb, ga, gb, xoa, xob, goa, gob,
                 aa, d1a, d3a, ab, d1b, d3b, aoa, d1oa, d3oa, aob, d1ob, d3ob, w1o, w3o, w2o):
    j = pl.program_id(0)
    all_hot = info[1] == j
    for m in range(2, 9):
        all_hot = all_hot & (info[m] == j)

    def run(first, second, cols):
        def part(n, q):
            x, g, a, d1, d3 = n
            return x[q, :, cols], g[q, :, cols], a[q], d1[q], d3[q]

        def products(parts):
            w1o[0, :, cols] = sum(mm(p[3], p[0], NN) for p in parts)
            w3o[0, :, cols] = sum(mm(p[4], p[0], NN) for p in parts)
            w2o[0, :, cols] = sum(mm(p[2], p[1], NN) for p in parts)

        main = [part(first[0], 0), part(second[0], 0)]

        @pl.when(all_hot)
        def _():
            products(main + [part(n[1], q) for n in (first, second) for q in range(2)])

        @pl.when(jnp.logical_not(all_hot))
        def _():
            products(main)
            for _, over, off in (first, second):

                def body(q, _):
                    h0, h1 = info[off + 2 * q], info[off + 2 * q + 1]

                    @pl.when((h0 == j) | (h1 == j))
                    def _():
                        x, g, a, d1, d3 = part(over, q)
                        row = lax.broadcasted_iota(jnp.int32, a.shape, 1)
                        mine = jnp.where(row < 128, h0, h1) == j

                        def keep(v):
                            return jnp.where(mine, v.astype(F32), 0.0).astype(BF16)

                        w1o[0, :, cols] += mm(keep(d1), x, NN)
                        w3o[0, :, cols] += mm(keep(d3), x, NN)
                        w2o[0, :, cols] += mm(keep(a), g, NN)

                    return 0

                lax.fori_loop(0, 2, body, 0)

    na = ((xa, ga, aa, d1a, d3a), (xoa, goa, aoa, d1oa, d3oa), 1)
    nb = ((xb, gb, ab, d1b, d3b), (xob, gob, aob, d1ob, d3ob), 5)

    def columns(h, _):
        cols = pl.ds(pl.multiple_of(h * 512, 512), 512)

        @pl.when(info[0] == 0)
        def _():
            run(na, nb, cols)

        @pl.when(info[0] == 1)
        def _():
            run(nb, na, cols)

        return 0

    lax.fori_loop(0, w1o.shape[2] // 512, columns, 0)


def wgrad(info, xa, ga, hid_a, xb, gb, hid_b, dim, ff):
    dc = 1024

    def over(off):
        def index(j, c, s):
            used = (s[off] == j) | (s[off + 1] == j) | (s[off + 2] == j) | (s[off + 3] == j)
            return 2, 0, jnp.where(used, c, 0)

        return pl.BlockSpec((2, 256, dc), index)

    main_blk = pl.BlockSpec((1, 256, dc), lambda j, c, s: (j, 0, c))
    hid_blk = pl.BlockSpec((1, ff, 256), lambda j, c, s: (j, 0, 0))
    hid_over = pl.BlockSpec((2, ff, 256), lambda j, c, s: (2, 0, 0))
    return pl.pallas_call(
        wgrad_kernel,
        grid_spec=pltpu.PrefetchScalarGridSpec(
            num_scalar_prefetch=1, grid=(4, dim // dc),
            in_specs=[main_blk] * 4 + [over(1), over(5)] * 2 + [hid_blk] * 6 + [hid_over] * 6,
            out_specs=[pl.BlockSpec((1, ff, dc), lambda j, c, s: (j, 0, c))] * 3),
        out_shape=[jax.ShapeDtypeStruct((4, ff, dim), F32)] * 3,
        compiler_params=pltpu.CompilerParams(vmem_limit_bytes=VMEM_LIMIT),
        cost_estimate=cost(3 * 2 * 3072 * dim * ff, 200e6),
        name="wgrad",
    )(info, xa, xb, ga, gb, xa, xb, ga, gb, *hid_a, *hid_b, *hid_a, *hid_b)


def solution(mesh):
    tok_spec = P(("dp", "ep"), None)
    exp_spec = P("ep", None, None)
    axes = ("dp", "ep")

    def shift(arr, dp_bit, ep_bits):
        pairs = [(s, (((s // 4) ^ dp_bit) * 4) + ((s % 4) ^ ep_bits)) for s in range(8)]
        return lax.ppermute(arr, axes, pairs)

    def device_step(x_loc, route_idx, w_router, w_gate, w_up, w_down, dy_loc):
        tok, dim = x_loc.shape
        ff = w_gate.shape[2]
        ep = lax.axis_index("ep")
        dp = lax.axis_index("dp")
        e0 = ep * 4
        w1t, w3t, w2 = jnp.swapaxes(w_gate, 1, 2), jnp.swapaxes(w_up, 1, 2), w_down

        order = jnp.arange(tok, dtype=jnp.int32)
        before = (order[:, None] < order[None, :]).astype(BF16)
        local = jnp.arange(4, dtype=jnp.int32)

        def tables(idx):
            picked = jnp.any(idx[:, None] == (e0 + local)[None, :, None, None], axis=2)
            ranks = jnp.dot(picked.reshape(16, tok).astype(BF16), before, preferred_element_type=F32)
            ranks = jnp.where(picked, ranks.reshape(4, 4, tok), -1.0)
            main = jnp.where((ranks >= 0) & (ranks < COLD), ranks + COLD * local.astype(F32)[None, :, None], -1.0)
            over = jnp.max(jnp.where(ranks >= COLD, ranks - COLD + 4 * COLD, -1.0), axis=1, keepdims=True)
            slots = jnp.concatenate([main, over, jnp.full((4, 3, tok), -1.0, F32)], axis=1)
            large = jnp.max(ranks, axis=2) >= COLD
            hot = jnp.min(jnp.where(large, local[None, :], 3), axis=1)
            first = jnp.arange(3, dtype=jnp.int32)
            first = first + (first >= hot[0])
            eidx = jnp.concatenate([first, hot[:1], hot])
            one = jnp.ones((), jnp.int32)
            act = jnp.stack([one, one, one, one, one, (hot[0] != hot[1]).astype(jnp.int32),
                             one, (hot[2] != hot[3]).astype(jnp.int32)])
            return ranks, slots, hot, eidx, act

        def gate_table(gates, ranks):
            mine = jnp.stack([lax.dynamic_slice_in_dim(v, e0, 4, axis=0) for v in gates])
            over = jnp.sum(jnp.where(ranks >= COLD, mine, 0.0), axis=1, keepdims=True)
            return jnp.concatenate([mine, over, jnp.zeros((4, 3, tok), F32)], axis=1)

        idx_t = route_idx.T
        idx_a = jnp.stack([idx_t] + [shift(idx_t, 0, k) for k in (1, 2, 3)])
        x_across = shift(x_loc, 0, 2)
        x_sib = shift(x_loc, 0, 1)
        x_y = shift(x_loc, 1, 0)
        g_across = shift(dy_loc, 0, 2)
        g_sib = shift(dy_loc, 0, 1)
        g_y = shift(dy_loc, 1, 0)
        idx_b = jnp.stack([shift(idx_t, 1, k) for k in range(4)])

        logits = jnp.dot(x_loc, w_router, preferred_element_type=F32)
        hit = route_idx[:, :, None] == jnp.arange(16, dtype=jnp.int32)
        chosen = jnp.sum(jnp.where(hit, logits[:, None, :], 0.0), axis=2)
        probs = jax.nn.softmax(chosen, axis=-1)
        gate_t = jnp.sum(jnp.where(hit, probs[:, :, None], 0.0), axis=1).T
        gates_a = [gate_t] + [shift(gate_t, 0, k) for k in (1, 2, 3)]
        gates_b = [shift(gate_t, 1, k) for k in range(4)]

        ranks_a, slots_a, hot_a, eidx_a, act_a = tables(idx_a)
        x_across_sib = shift(x_across, 0, 1)
        x_ya = shift(x_across, 1, 0)
        x_ys = shift(x_y, 0, 1)
        xa, = dispatch(slots_a, None, (x_loc, x_sib, x_across, x_across_sib), False)
        s_a, zu_a, sp_a, a_a = forward(eidx_a, act_a, xa, w1t, w3t)
        a_a, g_across, g_y, gates_a, gates_b, idx_b = lax.optimization_barrier((a_a, g_across, g_y, gates_a, gates_b, idx_b))
        ranks_b, slots_b, hot_b, eidx_b, act_b = tables(idx_b)
        g_across_sib = shift(g_across, 0, 1)
        g_ya = shift(g_across, 1, 0)
        g_ys = shift(g_y, 0, 1)
        da, ga = dispatch(slots_a, gate_table(gates_a, ranks_a), (dy_loc, g_sib, g_across, g_across_sib), True)
        d1_a, d3_a, q_a, d1r_a, d3r_a = hidden_grad(eidx_a, act_a, (da, ga), w2, (s_a, zu_a, sp_a, a_a))
        slots_t = jnp.swapaxes(slots_a, 1, 2)
        part = back(eidx_a, act_a, d1r_a, d3r_a, w1t, w3t, [slots_t[k] for k in range(4)])

        q_rows = q_a[:, 0, :]
        q_main = q_rows[:4].reshape(4, 4, COLD).transpose(1, 0, 2)
        q_over = q_rows[4:].reshape(4, OVER)
        r64 = jnp.arange(COLD, dtype=F32)
        r128 = jnp.arange(OVER, dtype=F32) + COLD
        q_tok = jnp.sum(jnp.where(ranks_a[..., None] == r64, q_main[:, :, None, :], 0.0), axis=3)
        q_tok = q_tok + jnp.sum(jnp.where(ranks_a[..., None] == r128, q_over[:, None, None, :], 0.0), axis=3)
        q_recv = [shift(q_tok[k], 0, k) for k in (1, 2, 3)]

        part_own, x_ya, q_recv = lax.optimization_barrier((part[0], x_ya, q_recv))
        x_yas = shift(x_ya, 0, 1)

        to_sib = shift(part[1], 0, 1)
        pair = part[2] + shift(part[3], 0, 1)

        q_back = jnp.stack([q_tok[0]] + q_recv)
        q16 = q_back[ep ^ local].reshape(16, tok)
        d_sel = gate_t * (q16 - jnp.sum(gate_t * q16, axis=0, keepdims=True))
        d_logits = d_sel.astype(BF16)
        gr = jnp.dot(d_logits, x_loc, preferred_element_type=F32)

        x_yas, pair, gr = lax.optimization_barrier((x_yas, pair, gr))
        from_across = shift(pair, 0, 2)
        gr_recv = shift(gr, 0, 1)
        xb, = dispatch(slots_b, None, (x_y, x_ys, x_ya, x_yas), False)
        s_b, zu_b, sp_b, a_b = forward(eidx_b, act_b, xb, w1t, w3t)
        a_b, s_b, g_ya, gr_recv = lax.optimization_barrier((a_b, s_b, g_ya, gr_recv))
        g_yas = shift(g_ya, 0, 1)
        gr = gr + gr_recv
        gr_recv = shift(gr, 1, 0)
        db, = dispatch(slots_b, gate_table(gates_b, ranks_b), (g_y, g_ys, g_ya, g_yas), False)
        d1_b, d3_b = hidden_grad(eidx_b, act_b, (db,), w2, (s_b, zu_b, sp_b))
        d1_b, gr_recv = lax.optimization_barrier((d1_b, gr_recv))
        gr = gr + gr_recv
        gr_recv = shift(gr, 0, 2)
        info = jnp.concatenate([dp[None].astype(jnp.int32), hot_a, hot_b])
        g1t, g3t, grad_down = wgrad(info, xa, da, (a_a, d1_a, d3_a), xb, db, (a_b, d1_b, d3_b), dim, ff)
        g1t, gr_recv, from_across, d_logits = lax.optimization_barrier((g1t, gr_recv, from_across, d_logits))
        grad_router = (gr + gr_recv).T
        du = lax.dot_general(d_logits, w_router, (((0,), (1,)), ((), ())), preferred_element_type=F32)
        grad_x = (part_own + to_sib + from_across + du).astype(BF16)
        return grad_x, jnp.swapaxes(g1t, 1, 2), jnp.swapaxes(g3t, 1, 2), grad_down, grad_router

    return jax.shard_map(device_step, mesh=mesh, in_specs=(tok_spec, tok_spec, P(), exp_spec, exp_spec, exp_spec, tok_spec), out_specs=(tok_spec, exp_spec, exp_spec, exp_spec, P()), check_vma=False)
```

```python
import functools

import jax
import jax.numpy as jnp
from jax import lax
from jax.experimental import pallas as pl
from jax.experimental.pallas import tpu as pltpu
from jax.sharding import PartitionSpec as P


COLD = 64
OVER = 128
VMEM_LIMIT = 62 * 1024 * 1024
F32 = jnp.float32
BF16 = jnp.bfloat16

NN = (((1,), (0,)), ((), ()))
NT = (((1,), (1,)), ((), ()))


def mm(a, b, dims):
    return lax.dot_general(a, b, dims, preferred_element_type=F32)


def tile_of(step, eidx):
    return jnp.where(step < 4, eidx[step], 4 + (step - 4) // 2)


def cost(flops, nbytes):
    return pl.CostEstimate(flops=int(flops), bytes_accessed=int(nbytes), transcendentals=0)


def expert_kernel(mode, n_c, dc, ring, eidx, act, slots, gates, *refs):
    has_x, has_g = mode != "grad", mode != "fwd"
    it = iter(refs)

    def take(n):
        return [next(it) for _ in range(n)]

    xs, gs = take(4 * has_x), take(4 * has_g)
    n_w = {"fwd": 2, "grad": 1, "both": 3}[mode]
    w_hbm = take(n_w)
    z_hbm = take(2) if mode == "grad" else []
    x_out, do_out = take(1 * has_x), take(1 * has_g)
    if mode == "fwd":
        z_hbm = take(2)
    hid, more = take(3 * has_g), take(3 * (mode == "grad"))
    acc = take(3 if mode == "both" else 2)
    zs = take(2 * (mode == "grad"))
    g_sc = take(1 * (mode == "grad"))
    wbuf, wsem = take(2)
    zsem = take(1 * (mode != "both"))
    c = pl.program_id(0)

    def w_copies(f, expert, slot):
        cols = pl.ds(pl.multiple_of((f // 4) * dc, dc), dc)
        return [pltpu.make_async_copy(w_hbm[n].at[expert, :, cols], wbuf.at[slot, n], wsem.at[slot, n])
                for n in range(n_w)]

    def ring_copies(f):
        return w_copies(f, eidx[lax.rem(f, 4)], lax.rem(f, ring))

    def z_copies(i):
        if mode == "fwd":
            return [pltpu.make_async_copy(acc[n].at[i], z_hbm[n].at[i], zsem[0].at[n, i]) for n in range(2)]
        return [pltpu.make_async_copy(z_hbm[n].at[i], zs[n].at[i], zsem[0].at[n, i]) for n in range(2)]

    def each_active(fn):
        for i in range(8):
            @pl.when(act[i] == 1)
            def _():
                fn(i)

    @pl.when(c == 0)
    def _():
        for f in range(ring - 1):
            for copy in ring_copies(jnp.int32(f)):
                copy.start()
        if mode == "grad":
            each_active(lambda i: [copy.start() for copy in z_copies(i)])

    def gather(k, row, gate, base, n, tile, lo):
        want = lax.broadcasted_iota(jnp.int32, (n, 256), 0) + base
        hit = row == want.astype(F32)
        sel = jnp.where(hit, 1.0, 0.0).astype(BF16)
        if has_x:
            x_out[0][tile, lo:lo + n, :] = mm(sel, xs[k][...], NN).astype(BF16)
        if has_g:
            rows = mm(sel, gs[k][...], NN)
            col = jnp.sum(jnp.where(hit, gate, 0.0), axis=1, keepdims=True)
            do_out[0][tile, lo:lo + n, :] = (col * rows).astype(BF16)
            if mode == "grad":
                g_sc[0][lo:lo + n, :] = rows.astype(BF16)

    def finish(i, tile, lo):
        n = 128
        cols = slice(lo, lo + n)
        if mode == "grad":
            z_gate, z_up, d_act = zs[0][i, :, cols], zs[1][i, :, cols], acc[0][i, :, cols]
        else:
            z_gate, z_up, d_act = acc[0][i, :, cols], acc[1][i, :, cols], acc[2][i, :, cols]
        sig = jax.nn.sigmoid(z_gate)
        silu = z_gate * sig
        a = (silu * z_up).astype(BF16)
        d1 = (d_act * z_up * sig * (1.0 + z_gate * (1.0 - sig))).astype(BF16)
        d3 = (d_act * silu).astype(BF16)
        for out, val in zip(hid, (a, d1, d3)):
            out[tile, :, cols] = val
        if mode == "grad":
            q_out, d1r_out, d3r_out = more
            q = jnp.sum(a.astype(F32) * acc[1][i, :, cols], axis=0, keepdims=True)
            q_out[tile, :, cols] = jnp.broadcast_to(q, (8, n))
            d1r_out[tile, cols, :] = d1.astype(F32).T.astype(BF16)
            d3r_out[tile, cols, :] = d3.astype(F32).T.astype(BF16)

    def step(i, _):
        expert = eidx[i]
        tile = tile_of(i, eidx)
        f = c * 4 + jnp.minimum(i, 3)
        stray = (i >= 4) & (expert != eidx[3])
        slot = jnp.where(stray, ring, lax.rem(f, ring))

        @pl.when(i < 4)
        def _():
            @pl.when(f + ring - 1 < 4 * n_c)
            def _():
                for copy in ring_copies(f + ring - 1):
                    copy.start()

            for k in range(4):
                gather(k, slots[k, pl.ds(expert, 1), :], gates[k, pl.ds(expert, 1), :], expert * COLD, COLD, tile, COLD * k)
            for copy in ring_copies(f):
                copy.wait()

        for q in range(2):
            @pl.when(i == 4 + 2 * q)
            def _():
                for half in range(2):
                    k = 2 * q + half
                    gather(k, slots[k, 4:5, :], gates[k, 4:5, :], 4 * COLD, OVER, 4 + q, OVER * half)

        @pl.when((act[i] == 1) & stray)
        def _():
            for copy in w_copies(f, expert, ring):
                copy.start()
            for copy in w_copies(f, expert, ring):
                copy.wait()

        @pl.when(act[i] == 1)
        def _():
            def add(ref, val):
                ref[i] = jnp.where(c == 0, 0.0, ref[i]) + val

            if has_x:
                x = x_out[0][tile]
                add(acc[0], mm(wbuf[slot, 0], x, NT))
                add(acc[1], mm(wbuf[slot, 1], x, NT))
            if has_g:
                add(acc[0 if mode == "grad" else 2], mm(wbuf[slot, n_w - 1], do_out[0][tile], NT))
            if mode == "grad":
                add(acc[1], mm(wbuf[slot, 0], g_sc[0][...], NT))

        @pl.when((act[i] == 1) & (c == n_c - 1))
        def _():
            if mode == "fwd":
                for copy in z_copies(i):
                    copy.start()
            else:
                if mode == "grad":
                    for copy in z_copies(i):
                        copy.wait()

                @pl.when((i != 5) & (i != 7))
                def _():
                    finish(i, tile, 0)

                finish(i, tile, 128)

        return 0

    lax.fori_loop(0, 8, step, 0)

    if mode == "fwd":
        @pl.when(c == n_c - 1)
        def _():
            each_active(lambda i: [copy.wait() for copy in z_copies(i)])


def experts(mode, eidx, act, slots, gates, xs, gs, weights, zs, dc, ring):
    has_x, has_g = mode != "grad", mode != "fwd"
    ff, dim = weights[0].shape[1:]
    n_c = dim // dc
    any_blk = pl.BlockSpec(memory_space=pl.ANY)
    small = pl.BlockSpec((4, 8, 256), lambda c, e, t: (0, 0, 0))
    v_blk = pl.BlockSpec((256, dc), lambda c, e, t: (0, c))

    def whole(d0, d1, dtype):
        return (jax.ShapeDtypeStruct((6, d0, d1), dtype),
                pl.BlockSpec((6, d0, d1), lambda c, e, t: (0, 0, 0), pipeline_mode=pl.Buffered(1)))

    outs = [(jax.ShapeDtypeStruct((6, 256, dim), BF16),
             pl.BlockSpec((6, 256, dc), lambda c, e, t: (0, 0, c)))] * (has_x + has_g)
    if mode == "fwd":
        outs += [(jax.ShapeDtypeStruct((8, ff, 256), F32), any_blk)] * 2
    if has_g:
        outs += [whole(ff, 256, BF16)] * 3
    if mode == "grad":
        outs += [whole(8, 256, F32), whole(256, ff, BF16), whole(256, ff, BF16)]
    n_acc = 3 if mode == "both" else 2
    scratch = [pltpu.VMEM((8, ff, 256), F32)] * (n_acc + len(zs))
    if mode == "grad":
        scratch.append(pltpu.VMEM((256, dc), BF16))
    scratch += [pltpu.VMEM((ring + 1, len(weights), ff, dc), BF16), pltpu.SemaphoreType.DMA((ring + 1, len(weights)))]
    if mode != "both":
        scratch.append(pltpu.SemaphoreType.DMA((2, 8)))
    n_v = len(xs) + len(gs)
    n_mm = 4 if mode == "both" else 2
    return pl.pallas_call(
        functools.partial(expert_kernel, mode, n_c, dc, ring),
        grid_spec=pltpu.PrefetchScalarGridSpec(
            num_scalar_prefetch=2, grid=(n_c,),
            in_specs=[small] * 2 + [v_blk] * n_v + [any_blk] * (len(weights) + len(zs)),
            out_specs=[o[1] for o in outs], scratch_shapes=scratch),
        out_shape=[o[0] for o in outs],
        compiler_params=pltpu.CompilerParams(vmem_limit_bytes=VMEM_LIMIT),
        cost_estimate=cost(n_mm * 2 * 1536 * dim * ff, 90e6),
    )(eidx, act, slots, gates, *xs, *gs, *weights, *zs)


def back_kernel(eidx, act, d1, d3, w1, w3, s0, s1, s2, s3, o0, o1, o2, o3, r_sc):
    step = pl.program_id(1)
    slots, outs = (s0, s1, s2, s3), (o0, o1, o2, o3)

    def rows(cols):
        r = (mm(d1[0], w1[0, :, cols], NN) + mm(d3[0], w3[0, :, cols], NN)).astype(BF16)

        @pl.when(step < 4)
        def _():
            lo = pl.multiple_of(eidx[step] * COLD, COLD)
            for k in range(4):
                r_sc[k, pl.ds(lo, COLD), cols] = r[COLD * k:COLD * (k + 1)]

        for q in range(2):
            @pl.when(step == 4 + 2 * q)
            def _():
                r_sc[2 * q, 256:384, cols] = r[0:128]

            @pl.when((step == 4 + 2 * q) | (step == 5 + 2 * q))
            def _():
                r_sc[2 * q + 1, 256:384, cols] = r[128:256]

    @pl.when(act[step] == 1)
    def _():
        def body(h, _):
            rows(pl.ds(pl.multiple_of(h * 1024, 1024), 1024))
            return 0

        lax.fori_loop(0, w1.shape[2] // 1024, body, 0)

    @pl.when(step == 7)
    def _():
        lane = lax.broadcasted_iota(jnp.int32, (256, 384), 1).astype(F32)
        for k in range(4):
            hit = lane == slots[k][:, 0:1]
            for m in range(1, 5):
                hit = hit | (lane == slots[k][:, m:m + 1])
            sel = jnp.where(hit, 1.0, 0.0).astype(BF16)
            outs[k][...] = mm(sel, r_sc[k], NN)


def back(eidx, act, d1, d3, w1t, w3t, slots):
    ff, dim = w1t.shape[1:]
    dc = 2048

    d_blk = pl.BlockSpec((1, 256, ff), lambda c, i, e, t: (tile_of(i, e), 0, 0))
    w_blk = pl.BlockSpec((1, ff, dc), lambda c, i, e, t: (e[i], 0, c))
    s_blk = pl.BlockSpec((256, 8), lambda c, i, e, t: (0, 0))
    o_blk = pl.BlockSpec((256, dc), lambda c, i, e, t: (0, c))
    return pl.pallas_call(
        back_kernel,
        grid_spec=pltpu.PrefetchScalarGridSpec(
            num_scalar_prefetch=2, grid=(dim // dc, 8),
            in_specs=[d_blk, d_blk, w_blk, w_blk] + [s_blk] * 4, out_specs=[o_blk] * 4,
            scratch_shapes=[pltpu.VMEM((4, 384, dc), BF16)]),
        out_shape=[jax.ShapeDtypeStruct((256, dim), F32)] * 4,
        compiler_params=pltpu.CompilerParams(vmem_limit_bytes=VMEM_LIMIT),
        cost_estimate=cost(2 * 2 * 1536 * dim * ff, 70e6),
        name="back",
    )(eidx, act, d1, d3, w1t, w3t, *slots)


def wgrad_kernel(info, xa, xb, ga, gb, xoa, xob, goa, gob,
                 aa, d1a, d3a, ab, d1b, d3b, aoa, d1oa, d3oa, aob, d1ob, d3ob, w1o, w3o, w2o):
    j = pl.program_id(0)
    all_hot = info[1] == j
    for m in range(2, 9):
        all_hot = all_hot & (info[m] == j)

    def run(first, second, cols):
        def part(n, q):
            x, g, a, d1, d3 = n
            return x[q, :, cols], g[q, :, cols], a[q], d1[q], d3[q]

        def products(parts):
            w1o[0, :, cols] = sum(mm(p[3], p[0], NN) for p in parts)
            w3o[0, :, cols] = sum(mm(p[4], p[0], NN) for p in parts)
            w2o[0, :, cols] = sum(mm(p[2], p[1], NN) for p in parts)

        main = [part(first[0], 0), part(second[0], 0)]

        @pl.when(all_hot)
        def _():
            products(main + [part(n[1], q) for n in (first, second) for q in range(2)])

        @pl.when(jnp.logical_not(all_hot))
        def _():
            products(main)
            for _, over, off in (first, second):

                def body(q, _):
                    h0, h1 = info[off + 2 * q], info[off + 2 * q + 1]

                    @pl.when((h0 == j) | (h1 == j))
                    def _():
                        x, g, a, d1, d3 = part(over, q)
                        row = lax.broadcasted_iota(jnp.int32, a.shape, 1)
                        mine = jnp.where(row < 128, h0, h1) == j

                        def keep(v):
                            return jnp.where(mine, v.astype(F32), 0.0).astype(BF16)

                        w1o[0, :, cols] += mm(keep(d1), x, NN)
                        w3o[0, :, cols] += mm(keep(d3), x, NN)
                        w2o[0, :, cols] += mm(keep(a), g, NN)

                    return 0

                lax.fori_loop(0, 2, body, 0)

    na = ((xa, ga, aa, d1a, d3a), (xoa, goa, aoa, d1oa, d3oa), 1)
    nb = ((xb, gb, ab, d1b, d3b), (xob, gob, aob, d1ob, d3ob), 5)

    def columns(h, _):
        cols = pl.ds(pl.multiple_of(h * 512, 512), 512)

        @pl.when(info[0] == 0)
        def _():
            run(na, nb, cols)

        @pl.when(info[0] == 1)
        def _():
            run(nb, na, cols)

        return 0

    lax.fori_loop(0, w1o.shape[2] // 512, columns, 0)


def wgrad(info, xa, ga, hid_a, xb, gb, hid_b, dim, ff):
    dc = 1024

    def over(off):
        def index(j, c, s):
            used = (s[off] == j) | (s[off + 1] == j) | (s[off + 2] == j) | (s[off + 3] == j)
            return 2, 0, jnp.where(used, c, 0)

        return pl.BlockSpec((2, 256, dc), index)

    main_blk = pl.BlockSpec((1, 256, dc), lambda j, c, s: (j, 0, c))
    hid_blk = pl.BlockSpec((1, ff, 256), lambda j, c, s: (j, 0, 0))
    hid_over = pl.BlockSpec((2, ff, 256), lambda j, c, s: (2, 0, 0))
    return pl.pallas_call(
        wgrad_kernel,
        grid_spec=pltpu.PrefetchScalarGridSpec(
            num_scalar_prefetch=1, grid=(4, dim // dc),
            in_specs=[main_blk] * 4 + [over(1), over(5)] * 2 + [hid_blk] * 6 + [hid_over] * 6,
            out_specs=[pl.BlockSpec((1, ff, dc), lambda j, c, s: (j, 0, c))] * 3),
        out_shape=[jax.ShapeDtypeStruct((4, ff, dim), F32)] * 3,
        compiler_params=pltpu.CompilerParams(vmem_limit_bytes=VMEM_LIMIT),
        cost_estimate=cost(3 * 2 * 3072 * dim * ff, 200e6),
        name="wgrad",
    )(info, xa, xb, ga, gb, xa, xb, ga, gb, *hid_a, *hid_b, *hid_a, *hid_b)


def solution(mesh):
    tok_spec = P(("dp", "ep"), None)
    exp_spec = P("ep", None, None)
    axes = ("dp", "ep")

    def shift(arr, dp_bit, ep_bits):
        pairs = [(s, (((s // 4) ^ dp_bit) * 4) + ((s % 4) ^ ep_bits)) for s in range(8)]
        return lax.ppermute(arr, axes, pairs)

    def device_step(x_loc, route_idx, w_router, w_gate, w_up, w_down, dy_loc):
        tok, dim = x_loc.shape
        ff = w_gate.shape[2]
        ep = lax.axis_index("ep")
        dp = lax.axis_index("dp")
        e0 = ep * 4
        w1t, w3t, w2 = jnp.swapaxes(w_gate, 1, 2), jnp.swapaxes(w_up, 1, 2), w_down

        order = jnp.arange(tok, dtype=jnp.int32)
        before = (order[:, None] < order[None, :]).astype(BF16)
        local = jnp.arange(4, dtype=jnp.int32)

        def tables(idx):
            picked = jnp.any(idx[:, None] == (e0 + local)[None, :, None, None], axis=2)
            ranks = jnp.dot(picked.reshape(16, tok).astype(BF16), before, preferred_element_type=F32)
            ranks = jnp.where(picked, ranks.reshape(4, 4, tok), -1.0)
            main = jnp.where((ranks >= 0) & (ranks < COLD), ranks + COLD * local.astype(F32)[None, :, None], -1.0)
            over = jnp.max(jnp.where(ranks >= COLD, ranks - COLD + 4 * COLD, -1.0), axis=1, keepdims=True)
            slots = jnp.concatenate([main, over, jnp.full((4, 3, tok), -1.0, F32)], axis=1)
            large = jnp.max(ranks, axis=2) >= COLD
            hot = jnp.min(jnp.where(large, local[None, :], 3), axis=1)
            first = jnp.arange(3, dtype=jnp.int32)
            first = first + (first >= hot[0])
            eidx = jnp.concatenate([first, hot[:1], hot])
            one = jnp.ones((), jnp.int32)
            act = jnp.stack([one, one, one, one, one, (hot[0] != hot[1]).astype(jnp.int32),
                             one, (hot[2] != hot[3]).astype(jnp.int32)])
            return ranks, slots, hot, eidx, act

        def gate_table(gates, ranks):
            mine = jnp.stack([lax.dynamic_slice_in_dim(v, e0, 4, axis=0) for v in gates])
            over = jnp.sum(jnp.where(ranks >= COLD, mine, 0.0), axis=1, keepdims=True)
            return jnp.concatenate([mine, over, jnp.zeros((4, 3, tok), F32)], axis=1)

        idx_t = route_idx.T
        idx_a = jnp.stack([idx_t] + [shift(idx_t, 0, k) for k in (1, 2, 3)])
        x_across = shift(x_loc, 0, 2)
        x_sib = shift(x_loc, 0, 1)
        x_y = shift(x_loc, 1, 0)
        g_across = shift(dy_loc, 0, 2)
        g_sib = shift(dy_loc, 0, 1)
        g_y = shift(dy_loc, 1, 0)
        idx_b = jnp.stack([shift(idx_t, 1, k) for k in range(4)])

        logits = jnp.dot(x_loc, w_router, preferred_element_type=F32)
        hit = route_idx[:, :, None] == jnp.arange(16, dtype=jnp.int32)
        chosen = jnp.sum(jnp.where(hit, logits[:, None, :], 0.0), axis=2)
        probs = jax.nn.softmax(chosen, axis=-1)
        gate_t = jnp.sum(jnp.where(hit, probs[:, :, None], 0.0), axis=1).T
        gates_a = [gate_t] + [shift(gate_t, 0, k) for k in (1, 2, 3)]
        gates_b = [shift(gate_t, 1, k) for k in range(4)]

        ranks_a, slots_a, hot_a, eidx_a, act_a = tables(idx_a)
        x_across_sib = shift(x_across, 0, 1)
        x_ya = shift(x_across, 1, 0)
        x_ys = shift(x_y, 0, 1)
        gate_a0 = jnp.zeros((4, 8, tok), F32)
        xa, z1_a, z3_a = experts("fwd", eidx_a, act_a, slots_a, gate_a0, (x_loc, x_sib, x_across, x_across_sib), (),
                                 (w1t, w3t), (), 1024, 4)
        z1_a, g_across, g_y, gates_a, gates_b, idx_b = lax.optimization_barrier((z1_a, g_across, g_y, gates_a, gates_b, idx_b))
        ranks_b, slots_b, hot_b, eidx_b, act_b = tables(idx_b)
        g_across_sib = shift(g_across, 0, 1)
        g_ya = shift(g_across, 1, 0)
        g_ys = shift(g_y, 0, 1)
        gate_a = gate_table(gates_a, ranks_a)
        da, a_a, d1_a, d3_a, q_a, d1r_a, d3r_a = experts(
            "grad", eidx_a, act_a, slots_a, gate_a, (), (dy_loc, g_sib, g_across, g_across_sib), (w2,), (z1_a, z3_a), 1024, 4)
        slots_t = jnp.swapaxes(slots_a, 1, 2)
        part = back(eidx_a, act_a, d1r_a, d3r_a, w1t, w3t, [slots_t[k] for k in range(4)])

        q_rows = q_a[:, 0, :]
        q_main = q_rows[:4].reshape(4, 4, COLD).transpose(1, 0, 2)
        q_over = q_rows[4:].reshape(4, OVER)
        r64 = jnp.arange(COLD, dtype=F32)
        r128 = jnp.arange(OVER, dtype=F32) + COLD
        q_tok = jnp.sum(jnp.where(ranks_a[..., None] == r64, q_main[:, :, None, :], 0.0), axis=3)
        q_tok = q_tok + jnp.sum(jnp.where(ranks_a[..., None] == r128, q_over[:, None, None, :], 0.0), axis=3)
        q_recv = [shift(q_tok[k], 0, k) for k in (1, 2, 3)]

        part_own, x_ya, g_ya, q_recv = lax.optimization_barrier((part[0], x_ya, g_ya, q_recv))
        x_yas = shift(x_ya, 0, 1)
        g_yas = shift(g_ya, 0, 1)
        gate_b = gate_table(gates_b, ranks_b)

        to_sib = shift(part[1], 0, 1)
        pair = part[2] + shift(part[3], 0, 1)

        q_back = jnp.stack([q_tok[0]] + q_recv)
        q16 = q_back[ep ^ local].reshape(16, tok)
        d_sel = gate_t * (q16 - jnp.sum(gate_t * q16, axis=0, keepdims=True))
        d_logits = d_sel.astype(BF16)
        gr = jnp.dot(d_logits, x_loc, preferred_element_type=F32)

        x_yas, g_yas, pair, gr = lax.optimization_barrier((x_yas, g_yas, pair, gr))
        from_across = shift(pair, 0, 2)
        gr = gr + shift(gr, 0, 1)
        gr_recv = shift(gr, 1, 0)
        xb, db, a_b, d1_b, d3_b = experts(
            "both", eidx_b, act_b, slots_b, gate_b, (x_y, x_ys, x_ya, x_yas), (g_y, g_ys, g_ya, g_yas),
            (w1t, w3t, w2), (), 512, 4)
        d1_b, gr_recv = lax.optimization_barrier((d1_b, gr_recv))
        gr = gr + gr_recv
        gr_recv = shift(gr, 0, 2)
        info = jnp.concatenate([dp[None].astype(jnp.int32), hot_a, hot_b])
        g1t, g3t, grad_down = wgrad(info, xa, da, (a_a, d1_a, d3_a), xb, db, (a_b, d1_b, d3_b), dim, ff)
        g1t, gr_recv, from_across, d_logits = lax.optimization_barrier((g1t, gr_recv, from_across, d_logits))
        grad_router = (gr + gr_recv).T
        du = lax.dot_general(d_logits, w_router, (((0,), (1,)), ((), ())), preferred_element_type=F32)
        grad_x = (part_own + to_sib + from_across + du).astype(BF16)
        return grad_x, jnp.swapaxes(g1t, 1, 2), jnp.swapaxes(g3t, 1, 2), grad_down, grad_router

    return jax.shard_map(device_step, mesh=mesh, in_specs=(tok_spec, tok_spec, P(), exp_spec, exp_spec, exp_spec, tok_spec), out_specs=(tok_spec, exp_spec, exp_spec, exp_spec, P()), check_vma=False)
```

```python
import functools

import jax
import jax.numpy as jnp
from jax import lax
from jax.experimental import pallas as pl
from jax.experimental.pallas import tpu as pltpu
from jax.sharding import PartitionSpec as P


COLD = 64
OVER = 128
VMEM_LIMIT = 62 * 1024 * 1024
F32 = jnp.float32
BF16 = jnp.bfloat16

NN = (((1,), (0,)), ((), ()))
NT = (((1,), (1,)), ((), ()))


def mm(a, b, dims):
    return lax.dot_general(a, b, dims, preferred_element_type=F32)


def tile_of(step, eidx):
    return jnp.where(step < 4, eidx[step], 4 + (step - 4) // 2)


def cost(flops, nbytes):
    return pl.CostEstimate(flops=int(flops), bytes_accessed=int(nbytes), transcendentals=0)


def expert_kernel(mode, n_c, dc, ring, eidx, act, slots, gates, *refs):
    has_x, has_g = mode != "grad", mode != "fwd"
    it = iter(refs)

    def take(n):
        return [next(it) for _ in range(n)]

    xs, gs = take(4 * has_x), take(4 * has_g)
    n_w = {"fwd": 2, "grad": 1, "both": 3}[mode]
    w_hbm = take(n_w)
    z_hbm = take(2) if mode == "grad" else []
    x_out, do_out = take(1 * has_x), take(1 * has_g)
    if mode == "fwd":
        z_hbm = take(2)
    hid, more = take(3 * has_g), take(3 * (mode == "grad"))
    acc = take(3 if mode == "both" else 2)
    zs = take(2 * (mode == "grad"))
    g_sc = take(1 * (mode == "grad"))
    sel, wbuf, wsem = take(3)
    zsem = take(1 * (mode != "both"))
    col = take(1 * has_g)
    c = pl.program_id(0)

    def w_copies(f, expert, slot):
        cols = pl.ds(pl.multiple_of((f // 4) * dc, dc), dc)
        return [pltpu.make_async_copy(w_hbm[n].at[expert, :, cols], wbuf.at[slot, n], wsem.at[slot, n])
                for n in range(n_w)]

    def ring_copies(f):
        return w_copies(f, eidx[lax.rem(f, 4)], lax.rem(f, ring))

    def z_copies(i):
        if mode == "fwd":
            return [pltpu.make_async_copy(acc[n].at[i], z_hbm[n].at[i], zsem[0].at[n, i]) for n in range(2)]
        return [pltpu.make_async_copy(z_hbm[n].at[i], zs[n].at[i], zsem[0].at[n, i]) for n in range(2)]

    def each_active(fn):
        for i in range(8):
            @pl.when(act[i] == 1)
            def _():
                fn(i)

    @pl.when(c == 0)
    def _():
        for f in range(ring - 1):
            for copy in ring_copies(jnp.int32(f)):
                copy.start()
        if mode == "grad":
            each_active(lambda i: [copy.start() for copy in z_copies(i)])

    @pl.when(c == 0)
    def _():
        for k in range(4):
            for m in range(5):
                n = OVER if m == 4 else COLD
                lo = COLD * m
                row = (lax.broadcasted_iota(jnp.int32, (n, 256), 0) + lo).astype(F32)
                hit = slots[k, m:m + 1, :] == row
                sel[k, lo:lo + n, :] = jnp.where(hit, 1.0, 0.0).astype(BF16)
                if has_g:
                    col[0][k, lo:lo + n, :] = jnp.sum(jnp.where(hit, gates[k, m:m + 1, :], 0.0), axis=1, keepdims=True)

    def put(out, k, rows):
        for j in range(4):
            out[j, COLD * k:COLD * (k + 1), :] = rows[COLD * j:COLD * (j + 1)]
        out[4 + k // 2, OVER * (k % 2):OVER * (k % 2) + OVER, :] = rows[256:384]

    for k in range(4):
        if has_x:
            put(x_out[0], k, mm(sel[k], xs[k][...], NN).astype(BF16))
        if has_g:
            rows = mm(sel[k], gs[k][...], NN)
            put(do_out[0], k, (col[0][k] * rows).astype(BF16))
            if mode == "grad":
                put(g_sc[0], k, rows.astype(BF16))

    def finish(i, tile, lo):
        n = 128
        cols = slice(lo, lo + n)
        if mode == "grad":
            z_gate, z_up, d_act = zs[0][i, :, cols], zs[1][i, :, cols], acc[0][i, :, cols]
        else:
            z_gate, z_up, d_act = acc[0][i, :, cols], acc[1][i, :, cols], acc[2][i, :, cols]
        sig = jax.nn.sigmoid(z_gate)
        silu = z_gate * sig
        a = (silu * z_up).astype(BF16)
        d1 = (d_act * z_up * sig * (1.0 + z_gate * (1.0 - sig))).astype(BF16)
        d3 = (d_act * silu).astype(BF16)
        for out, val in zip(hid, (a, d1, d3)):
            out[tile, :, cols] = val
        if mode == "grad":
            q_out, d1r_out, d3r_out = more
            q = jnp.sum(a.astype(F32) * acc[1][i, :, cols], axis=0, keepdims=True)
            q_out[tile, :, cols] = jnp.broadcast_to(q, (8, n))
            d1r_out[tile, cols, :] = d1.astype(F32).T.astype(BF16)
            d3r_out[tile, cols, :] = d3.astype(F32).T.astype(BF16)

    def step(i, _):
        expert = eidx[i]
        tile = tile_of(i, eidx)
        f = c * 4 + jnp.minimum(i, 3)
        stray = (i >= 4) & (expert != eidx[3])
        slot = jnp.where(stray, ring, lax.rem(f, ring))

        @pl.when(i < 4)
        def _():
            @pl.when(f + ring - 1 < 4 * n_c)
            def _():
                for copy in ring_copies(f + ring - 1):
                    copy.start()

            for copy in ring_copies(f):
                copy.wait()

        @pl.when((act[i] == 1) & stray)
        def _():
            for copy in w_copies(f, expert, ring):
                copy.start()
            for copy in w_copies(f, expert, ring):
                copy.wait()

        @pl.when(act[i] == 1)
        def _():
            def add(ref, val):
                ref[i] = jnp.where(c == 0, 0.0, ref[i]) + val

            if has_x:
                x = x_out[0][tile]
                add(acc[0], mm(wbuf[slot, 0], x, NT))
                add(acc[1], mm(wbuf[slot, 1], x, NT))
            if has_g:
                add(acc[0 if mode == "grad" else 2], mm(wbuf[slot, n_w - 1], do_out[0][tile], NT))
            if mode == "grad":
                add(acc[1], mm(wbuf[slot, 0], g_sc[0][tile], NT))

        @pl.when((act[i] == 1) & (c == n_c - 1))
        def _():
            if mode == "fwd":
                for copy in z_copies(i):
                    copy.start()
            else:
                if mode == "grad":
                    for copy in z_copies(i):
                        copy.wait()

                @pl.when((i != 5) & (i != 7))
                def _():
                    finish(i, tile, 0)

                finish(i, tile, 128)

        return 0

    lax.fori_loop(0, 8, step, 0)

    if mode == "fwd":
        @pl.when(c == n_c - 1)
        def _():
            each_active(lambda i: [copy.wait() for copy in z_copies(i)])


def experts(mode, eidx, act, slots, gates, xs, gs, weights, zs, dc, ring):
    has_x, has_g = mode != "grad", mode != "fwd"
    ff, dim = weights[0].shape[1:]
    n_c = dim // dc
    any_blk = pl.BlockSpec(memory_space=pl.ANY)
    small = pl.BlockSpec((4, 8, 256), lambda c, e, t: (0, 0, 0))
    v_blk = pl.BlockSpec((256, dc), lambda c, e, t: (0, c))

    def whole(d0, d1, dtype):
        return (jax.ShapeDtypeStruct((6, d0, d1), dtype),
                pl.BlockSpec((6, d0, d1), lambda c, e, t: (0, 0, 0), pipeline_mode=pl.Buffered(1)))

    outs = [(jax.ShapeDtypeStruct((6, 256, dim), BF16),
             pl.BlockSpec((6, 256, dc), lambda c, e, t: (0, 0, c)))] * (has_x + has_g)
    if mode == "fwd":
        outs += [(jax.ShapeDtypeStruct((8, ff, 256), F32), any_blk)] * 2
    if has_g:
        outs += [whole(ff, 256, BF16)] * 3
    if mode == "grad":
        outs += [whole(8, 256, F32), whole(256, ff, BF16), whole(256, ff, BF16)]
    n_acc = 3 if mode == "both" else 2
    scratch = [pltpu.VMEM((8, ff, 256), F32)] * (n_acc + len(zs))
    if mode == "grad":
        scratch.append(pltpu.VMEM((6, 256, dc), BF16))
    scratch += [pltpu.VMEM((4, 384, 256), BF16), pltpu.VMEM((ring + 1, len(weights), ff, dc), BF16), pltpu.SemaphoreType.DMA((ring + 1, len(weights)))]
    if mode != "both":
        scratch.append(pltpu.SemaphoreType.DMA((2, 8)))
    if has_g:
        scratch.append(pltpu.VMEM((4, 384, 1), F32))
    n_v = len(xs) + len(gs)
    n_mm = 4 if mode == "both" else 2
    return pl.pallas_call(
        functools.partial(expert_kernel, mode, n_c, dc, ring),
        grid_spec=pltpu.PrefetchScalarGridSpec(
            num_scalar_prefetch=2, grid=(n_c,),
            in_specs=[small] * 2 + [v_blk] * n_v + [any_blk] * (len(weights) + len(zs)),
            out_specs=[o[1] for o in outs], scratch_shapes=scratch),
        out_shape=[o[0] for o in outs],
        compiler_params=pltpu.CompilerParams(vmem_limit_bytes=VMEM_LIMIT),
        cost_estimate=cost(n_mm * 2 * 1536 * dim * ff, 90e6),
    )(eidx, act, slots, gates, *xs, *gs, *weights, *zs)


def back_kernel(n_c, dc, ring, eidx, act, d1, d3, w1_hbm, w3_hbm, s0, s1, s2, s3, o0, o1, o2, o3, r_sc, sel, wbuf, wsem):
    c = pl.program_id(0)
    slots, outs = (s0, s1, s2, s3), (o0, o1, o2, o3)

    def w_copies(f, expert, slot):
        cols = pl.ds(pl.multiple_of((f // 4) * dc, dc), dc)
        return [pltpu.make_async_copy(w.at[expert, :, cols], wbuf.at[slot, n], wsem.at[slot, n])
                for n, w in enumerate((w1_hbm, w3_hbm))]

    def ring_copies(f):
        return w_copies(f, eidx[lax.rem(f, 4)], lax.rem(f, ring))

    @pl.when(c == 0)
    def _():
        for f in range(ring - 1):
            for copy in ring_copies(jnp.int32(f)):
                copy.start()
        lane = lax.broadcasted_iota(jnp.int32, (256, 384), 1).astype(F32)
        for k in range(4):
            hit = lane == slots[k][:, 0:1]
            for m in range(1, 5):
                hit = hit | (lane == slots[k][:, m:m + 1])
            sel[k] = jnp.where(hit, 1.0, 0.0).astype(BF16)

    def step(i, _):
        expert = eidx[i]
        tile = tile_of(i, eidx)
        f = c * 4 + jnp.minimum(i, 3)
        stray = (i >= 4) & (expert != eidx[3])
        slot = jnp.where(stray, ring, lax.rem(f, ring))

        @pl.when(i < 4)
        def _():
            @pl.when(f + ring - 1 < 4 * n_c)
            def _():
                for copy in ring_copies(f + ring - 1):
                    copy.start()

            for copy in ring_copies(f):
                copy.wait()

        @pl.when((act[i] == 1) & stray)
        def _():
            for copy in w_copies(f, expert, ring):
                copy.start()
            for copy in w_copies(f, expert, ring):
                copy.wait()

        @pl.when(act[i] == 1)
        def _():
            r = (mm(d1[tile], wbuf[slot, 0], NN) + mm(d3[tile], wbuf[slot, 1], NN)).astype(BF16)

            @pl.when(i < 4)
            def _():
                lo = pl.multiple_of(expert * COLD, COLD)
                for k in range(4):
                    r_sc[k, pl.ds(lo, COLD), :] = r[COLD * k:COLD * (k + 1)]

            for q in range(2):
                @pl.when(i == 4 + 2 * q)
                def _():
                    r_sc[2 * q, 256:384, :] = r[0:128]

                @pl.when((i == 4 + 2 * q) | (i == 5 + 2 * q))
                def _():
                    r_sc[2 * q + 1, 256:384, :] = r[128:256]

        return 0

    lax.fori_loop(0, 8, step, 0)
    for k in range(4):
        outs[k][...] = mm(sel[k], r_sc[k], NN)


def back(eidx, act, d1, d3, w1t, w3t, slots):
    ff, dim = w1t.shape[1:]
    dc, ring = 1024, 4
    n_c = dim // dc
    d_blk = pl.BlockSpec((6, 256, ff), lambda c, e, t: (0, 0, 0), pipeline_mode=pl.Buffered(1))
    any_blk = pl.BlockSpec(memory_space=pl.ANY)
    s_blk = pl.BlockSpec((256, 8), lambda c, e, t: (0, 0))
    return pl.pallas_call(
        functools.partial(back_kernel, n_c, dc, ring),
        grid_spec=pltpu.PrefetchScalarGridSpec(
            num_scalar_prefetch=2, grid=(n_c,),
            in_specs=[d_blk, d_blk, any_blk, any_blk] + [s_blk] * 4,
            out_specs=[pl.BlockSpec((256, dc), lambda c, e, t: (0, c))] * 4,
            scratch_shapes=[pltpu.VMEM((4, 384, dc), BF16), pltpu.VMEM((4, 256, 384), BF16),
                            pltpu.VMEM((ring + 1, 2, ff, dc), BF16), pltpu.SemaphoreType.DMA((ring + 1, 2))]),
        out_shape=[jax.ShapeDtypeStruct((256, dim), F32)] * 4,
        compiler_params=pltpu.CompilerParams(vmem_limit_bytes=VMEM_LIMIT),
        cost_estimate=cost(2 * 2 * 1536 * dim * ff, 70e6),
        name="back",
    )(eidx, act, d1, d3, w1t, w3t, *slots)


def wgrad_kernel(info, xa, xb, ga, gb, xoa, xob, goa, gob,
                 aa, d1a, d3a, ab, d1b, d3b, w1o, w3o, w2o):
    j = pl.program_id(1)
    all_hot = info[1] == j
    for m in range(2, 9):
        all_hot = all_hot & (info[m] == j)

    def run(first, second, cols):
        def part(n, q):
            (x, g, a, d1, d3), tile = n
            return x[q, :, cols], g[q, :, cols], a[tile + q], d1[tile + q], d3[tile + q]

        def products(parts):
            w1o[0, :, cols] = sum(mm(p[3], p[0], NN) for p in parts)
            w3o[0, :, cols] = sum(mm(p[4], p[0], NN) for p in parts)
            w2o[0, :, cols] = sum(mm(p[2], p[1], NN) for p in parts)

        main = [part(first[0], 0), part(second[0], 0)]

        @pl.when(all_hot)
        def _():
            products(main + [part(n[1], q) for n in (first, second) for q in range(2)])

        @pl.when(jnp.logical_not(all_hot))
        def _():
            products(main)
            for _, over, off in (first, second):

                def body(q, _):
                    h0, h1 = info[off + 2 * q], info[off + 2 * q + 1]

                    @pl.when((h0 == j) | (h1 == j))
                    def _():
                        x, g, a, d1, d3 = part(over, q)
                        row = lax.broadcasted_iota(jnp.int32, a.shape, 1)
                        mine = jnp.where(row < 128, h0, h1) == j

                        def keep(v):
                            return jnp.where(mine, v.astype(F32), 0.0).astype(BF16)

                        w1o[0, :, cols] += mm(keep(d1), x, NN)
                        w3o[0, :, cols] += mm(keep(d3), x, NN)
                        w2o[0, :, cols] += mm(keep(a), g, NN)

                    return 0

                lax.fori_loop(0, 2, body, 0)

    na = (((xa, ga, aa, d1a, d3a), j), ((xoa, goa, aa, d1a, d3a), 4), 1)
    nb = (((xb, gb, ab, d1b, d3b), j), ((xob, gob, ab, d1b, d3b), 4), 5)

    def columns(h, _):
        cols = pl.ds(pl.multiple_of(h * 512, 512), 512)

        @pl.when(info[0] == 0)
        def _():
            run(na, nb, cols)

        @pl.when(info[0] == 1)
        def _():
            run(nb, na, cols)

        return 0

    lax.fori_loop(0, w1o.shape[2] // 512, columns, 0)


def wgrad(info, xa, ga, hid_a, xb, gb, hid_b, dim, ff):
    dc = 1024

    main_blk = pl.BlockSpec((1, 256, dc), lambda c, j, s: (j, 0, c))
    over_blk = pl.BlockSpec((2, 256, dc), lambda c, j, s: (2, 0, c))
    hid_blk = pl.BlockSpec((6, ff, 256), lambda c, j, s: (0, 0, 0), pipeline_mode=pl.Buffered(1))
    return pl.pallas_call(
        wgrad_kernel,
        grid_spec=pltpu.PrefetchScalarGridSpec(
            num_scalar_prefetch=1, grid=(dim // dc, 4),
            in_specs=[main_blk] * 4 + [over_blk] * 4 + [hid_blk] * 6,
            out_specs=[pl.BlockSpec((1, ff, dc), lambda c, j, s: (j, 0, c))] * 3),
        out_shape=[jax.ShapeDtypeStruct((4, ff, dim), F32)] * 3,
        compiler_params=pltpu.CompilerParams(vmem_limit_bytes=VMEM_LIMIT),
        cost_estimate=cost(3 * 2 * 3072 * dim * ff, 200e6),
        name="wgrad",
    )(info, xa, xb, ga, gb, xa, xb, ga, gb, *hid_a, *hid_b)


def solution(mesh):
    tok_spec = P(("dp", "ep"), None)
    exp_spec = P("ep", None, None)
    axes = ("dp", "ep")

    def shift(arr, dp_bit, ep_bits):
        pairs = [(s, (((s // 4) ^ dp_bit) * 4) + ((s % 4) ^ ep_bits)) for s in range(8)]
        return lax.ppermute(arr, axes, pairs)

    def device_step(x_loc, route_idx, w_router, w_gate, w_up, w_down, dy_loc):
        tok, dim = x_loc.shape
        ff = w_gate.shape[2]
        ep = lax.axis_index("ep")
        dp = lax.axis_index("dp")
        e0 = ep * 4
        w1t, w3t, w2 = jnp.swapaxes(w_gate, 1, 2), jnp.swapaxes(w_up, 1, 2), w_down

        order = jnp.arange(tok, dtype=jnp.int32)
        before = (order[:, None] < order[None, :]).astype(BF16)
        local = jnp.arange(4, dtype=jnp.int32)

        def tables(idx):
            picked = jnp.any(idx[:, None] == (e0 + local)[None, :, None, None], axis=2)
            ranks = jnp.dot(picked.reshape(16, tok).astype(BF16), before, preferred_element_type=F32)
            ranks = jnp.where(picked, ranks.reshape(4, 4, tok), -1.0)
            main = jnp.where((ranks >= 0) & (ranks < COLD), ranks + COLD * local.astype(F32)[None, :, None], -1.0)
            over = jnp.max(jnp.where(ranks >= COLD, ranks - COLD + 4 * COLD, -1.0), axis=1, keepdims=True)
            slots = jnp.concatenate([main, over, jnp.full((4, 3, tok), -1.0, F32)], axis=1)
            large = jnp.max(ranks, axis=2) >= COLD
            hot = jnp.min(jnp.where(large, local[None, :], 3), axis=1)
            first = jnp.arange(3, dtype=jnp.int32)
            first = first + (first >= hot[0])
            eidx = jnp.concatenate([first, hot[:1], hot])
            one = jnp.ones((), jnp.int32)
            act = jnp.stack([one, one, one, one, one, (hot[0] != hot[1]).astype(jnp.int32),
                             one, (hot[2] != hot[3]).astype(jnp.int32)])
            return ranks, slots, hot, eidx, act

        def gate_table(gates, ranks):
            mine = jnp.stack([lax.dynamic_slice_in_dim(v, e0, 4, axis=0) for v in gates])
            over = jnp.sum(jnp.where(ranks >= COLD, mine, 0.0), axis=1, keepdims=True)
            return jnp.concatenate([mine, over, jnp.zeros((4, 3, tok), F32)], axis=1)

        idx_t = route_idx.T
        idx_a = jnp.stack([idx_t] + [shift(idx_t, 0, k) for k in (1, 2, 3)])
        x_across = shift(x_loc, 0, 2)
        x_sib = shift(x_loc, 0, 1)
        x_y = shift(x_loc, 1, 0)
        g_across = shift(dy_loc, 0, 2)
        g_sib = shift(dy_loc, 0, 1)
        g_y = shift(dy_loc, 1, 0)
        idx_b = jnp.stack([shift(idx_t, 1, k) for k in range(4)])

        logits = jnp.dot(x_loc, w_router, preferred_element_type=F32)
        hit = route_idx[:, :, None] == jnp.arange(16, dtype=jnp.int32)
        chosen = jnp.sum(jnp.where(hit, logits[:, None, :], 0.0), axis=2)
        probs = jax.nn.softmax(chosen, axis=-1)
        gate_t = jnp.sum(jnp.where(hit, probs[:, :, None], 0.0), axis=1).T
        gates_a = [gate_t] + [shift(gate_t, 0, k) for k in (1, 2, 3)]
        gates_b = [shift(gate_t, 1, k) for k in range(4)]

        ranks_a, slots_a, hot_a, eidx_a, act_a = tables(idx_a)
        x_across_sib = shift(x_across, 0, 1)
        x_ya = shift(x_across, 1, 0)
        x_ys = shift(x_y, 0, 1)
        gate_a0 = jnp.zeros((4, 8, tok), F32)
        xa, z1_a, z3_a = experts("fwd", eidx_a, act_a, slots_a, gate_a0, (x_loc, x_sib, x_across, x_across_sib), (),
                                 (w1t, w3t), (), 2048, 3)
        z1_a, g_across, g_y, gates_a, gates_b, idx_b = lax.optimization_barrier((z1_a, g_across, g_y, gates_a, gates_b, idx_b))
        ranks_b, slots_b, hot_b, eidx_b, act_b = tables(idx_b)
        g_across_sib = shift(g_across, 0, 1)
        g_ya = shift(g_across, 1, 0)
        g_ys = shift(g_y, 0, 1)
        gate_a = gate_table(gates_a, ranks_a)
        da, a_a, d1_a, d3_a, q_a, d1r_a, d3r_a = experts(
            "grad", eidx_a, act_a, slots_a, gate_a, (), (dy_loc, g_sib, g_across, g_across_sib), (w2,), (z1_a, z3_a), 1024, 4)
        slots_t = jnp.swapaxes(slots_a, 1, 2)
        part = back(eidx_a, act_a, d1r_a, d3r_a, w1t, w3t, [slots_t[k] for k in range(4)])

        q_rows = q_a[:, 0, :]
        q_main = q_rows[:4].reshape(4, 4, COLD).transpose(1, 0, 2)
        q_over = q_rows[4:].reshape(4, OVER)
        r64 = jnp.arange(COLD, dtype=F32)
        r128 = jnp.arange(OVER, dtype=F32) + COLD
        q_tok = jnp.sum(jnp.where(ranks_a[..., None] == r64, q_main[:, :, None, :], 0.0), axis=3)
        q_tok = q_tok + jnp.sum(jnp.where(ranks_a[..., None] == r128, q_over[:, None, None, :], 0.0), axis=3)
        q_recv = [shift(q_tok[k], 0, k) for k in (1, 2, 3)]

        part_own, x_ya, g_ya, q_recv = lax.optimization_barrier((part[0], x_ya, g_ya, q_recv))
        x_yas = shift(x_ya, 0, 1)
        g_yas = shift(g_ya, 0, 1)
        gate_b = gate_table(gates_b, ranks_b)

        to_sib = shift(part[1], 0, 1)
        pair = part[2] + shift(part[3], 0, 1)

        q_back = jnp.stack([q_tok[0]] + q_recv)
        q16 = q_back[ep ^ local].reshape(16, tok)
        d_sel = gate_t * (q16 - jnp.sum(gate_t * q16, axis=0, keepdims=True))
        d_logits = d_sel.astype(BF16)
        gr = jnp.dot(d_logits, x_loc, preferred_element_type=F32)

        x_yas, g_yas, pair, gr = lax.optimization_barrier((x_yas, g_yas, pair, gr))
        from_across = shift(pair, 0, 2)
        gr = gr + shift(gr, 0, 1)
        gr_recv = shift(gr, 1, 0)
        xb, db, a_b, d1_b, d3_b = experts(
            "both", eidx_b, act_b, slots_b, gate_b, (x_y, x_ys, x_ya, x_yas), (g_y, g_ys, g_ya, g_yas),
            (w1t, w3t, w2), (), 512, 4)
        d1_b, gr_recv = lax.optimization_barrier((d1_b, gr_recv))
        gr = gr + gr_recv
        gr_recv = shift(gr, 0, 2)
        info = jnp.concatenate([dp[None].astype(jnp.int32), hot_a, hot_b])
        g1t, g3t, grad_down = wgrad(info, xa, da, (a_a, d1_a, d3_a), xb, db, (a_b, d1_b, d3_b), dim, ff)
        g1t, gr_recv, from_across, d_logits = lax.optimization_barrier((g1t, gr_recv, from_across, d_logits))
        grad_router = (gr + gr_recv).T
        du = lax.dot_general(d_logits, w_router, (((0,), (1,)), ((), ())), preferred_element_type=F32)
        grad_x = (part_own + to_sib + from_across + du).astype(BF16)
        return grad_x, jnp.swapaxes(g1t, 1, 2), jnp.swapaxes(g3t, 1, 2), grad_down, grad_router

    return jax.shard_map(device_step, mesh=mesh, in_specs=(tok_spec, tok_spec, P(), exp_spec, exp_spec, exp_spec, tok_spec), out_specs=(tok_spec, exp_spec, exp_spec, exp_spec, P()), check_vma=False)
```

```python
import functools

import jax
import jax.numpy as jnp
from jax import lax
from jax.experimental import pallas as pl
from jax.experimental.pallas import tpu as pltpu
from jax.sharding import PartitionSpec as P


FOUR = range(4)
ORIGIN = (0, 0, 0)
COLD = 64
OVER = 128
VMEM_LIMIT = 62 * 1024 * 1024
F32 = jnp.float32
BF16 = jnp.bfloat16

NN = (((1,), (0,)), ((), ()))
NT = (((1,), (1,)), ((), ()))


def mm(a, b, dims):
    return lax.dot_general(a, b, dims, preferred_element_type=F32)


def tile_of(step, eidx):
    return jnp.where(step < 4, eidx[step], 4 + (step - 4) // 2)


def cost(flops, nbytes):
    return pl.CostEstimate(flops=int(flops), bytes_accessed=int(nbytes), transcendentals=0)


def expert_kernel(mode, n_c, dc, ring, eidx, act, slots, gates, *refs):
    has_x, has_g = mode != "grad", mode != "fwd"
    it = iter(refs)

    def take(n):
        return [next(it) for _ in range(n)]

    xs, gs = take(4 * has_x), take(4 * has_g)
    n_w = {"fwd": 2, "grad": 1, "both": 3}[mode]
    w_hbm = take(n_w)
    z_hbm = take(2) if mode == "grad" else []
    x_out, do_out = take(1 * has_x), take(1 * has_g)
    if mode == "fwd":
        z_hbm = take(2)
    hid_hbm = take(3 * has_g) + take(3 * (mode == "grad"))
    acc = take(3 if mode == "both" else 2)
    zs = take(2 * (mode == "grad"))
    g_sc = take(1 * (mode == "grad"))
    sel, wbuf, wsem = take(3)
    zsem = take(1 * (mode != "both"))
    col = take(1 * has_g)
    hid, more = take(3 * has_g), take(3 * (mode == "grad"))
    hsem = take(1 * has_g)
    c = pl.program_id(0)

    def w_copies(f, expert, slot):
        cols = pl.ds(pl.multiple_of((f // 4) * dc, dc), dc)
        return [pltpu.make_async_copy(w_hbm[n].at[expert, :, cols], wbuf.at[slot, n], wsem.at[slot, n])
                for n in range(n_w)]

    def ring_copies(f):
        return w_copies(f, eidx[lax.rem(f, 4)], lax.rem(f, ring))

    def z_copies(i):
        if mode == "fwd":
            return [pltpu.make_async_copy(acc[n].at[i], z_hbm[n].at[i], zsem[0].at[n, i]) for n in range(2)]
        return [pltpu.make_async_copy(z_hbm[n].at[i], zs[n].at[i], zsem[0].at[n, i]) for n in range(2)]

    def hid_copies(tile):
        return [pltpu.make_async_copy(v.at[tile], o.at[tile], hsem[0].at[n, tile])
                for n, (v, o) in enumerate(zip(hid + more, hid_hbm))]

    def each_active(fn):
        for i in range(8):
            @pl.when(act[i] == 1)
            def _():
                fn(i)

    @pl.when(c == 0)
    def _():
        for f in range(ring - 1):
            for copy in ring_copies(jnp.int32(f)):
                copy.start()
        if mode == "grad":
            each_active(lambda i: [copy.start() for copy in z_copies(i)])

    @pl.when(c == 0)
    def _():
        for k in FOUR:
            for m in range(5):
                n = OVER if m == 4 else COLD
                lo = COLD * m
                row = (lax.broadcasted_iota(jnp.int32, (n, 256), 0) + lo).astype(F32)
                hit = slots[k, m:m + 1, :] == row
                sel[k, lo:lo + n, :] = jnp.where(hit, 1.0, 0.0).astype(BF16)
                if has_g:
                    col[0][k, lo:lo + n, :] = jnp.sum(jnp.where(hit, gates[k, m:m + 1, :], 0.0), axis=1, keepdims=True)

    def put(out, k, rows):
        for j in FOUR:
            out[j, COLD * k:COLD * (k + 1), :] = rows[COLD * j:COLD * (j + 1)]
        out[4 + k // 2, OVER * (k % 2):OVER * (k % 2) + OVER, :] = rows[256:384]

    for k in FOUR:
        if has_x:
            put(x_out[0], k, mm(sel[k], xs[k][...], NN).astype(BF16))
        if has_g:
            rows = mm(sel[k], gs[k][...], NN)
            put(do_out[0], k, (col[0][k] * rows).astype(BF16))
            if mode == "grad":
                put(g_sc[0], k, rows.astype(BF16))

    def finish(i, tile, lo):
        n = 128
        cols = slice(lo, lo + n)
        if mode == "grad":
            z_gate, z_up, d_act = zs[0][i, :, cols], zs[1][i, :, cols], acc[0][i, :, cols]
        else:
            z_gate, z_up, d_act = acc[0][i, :, cols], acc[1][i, :, cols], acc[2][i, :, cols]
        sig = jax.nn.sigmoid(z_gate)
        silu = z_gate * sig
        a = (silu * z_up).astype(BF16)
        d1 = (d_act * z_up * sig * (1.0 + z_gate * (1.0 - sig))).astype(BF16)
        d3 = (d_act * silu).astype(BF16)
        for out, val in zip(hid, (a, d1, d3)):
            out[tile, :, cols] = val
        if mode == "grad":
            q_out, d1r_out, d3r_out = more
            q = jnp.sum(a.astype(F32) * acc[1][i, :, cols], axis=0, keepdims=True)
            q_out[tile, :, cols] = jnp.broadcast_to(q, (8, n))
            d1r_out[tile, cols, :] = d1.astype(F32).T.astype(BF16)
            d3r_out[tile, cols, :] = d3.astype(F32).T.astype(BF16)

    def step(i, _):
        expert = eidx[i]
        tile = tile_of(i, eidx)
        f = c * 4 + jnp.minimum(i, 3)
        stray = (i >= 4) & (expert != eidx[3])
        slot = jnp.where(stray, ring, lax.rem(f, ring))

        @pl.when(i < 4)
        def _():
            @pl.when(f + ring - 1 < 4 * n_c)
            def _():
                for copy in ring_copies(f + ring - 1):
                    copy.start()

            for copy in ring_copies(f):
                copy.wait()

        @pl.when((act[i] == 1) & stray)
        def _():
            for copy in w_copies(f, expert, ring):
                copy.start()
            for copy in w_copies(f, expert, ring):
                copy.wait()

        @pl.when(act[i] == 1)
        def _():
            def add(ref, val):
                ref[i] = jnp.where(c == 0, 0.0, ref[i]) + val

            if has_x:
                x = x_out[0][tile]
                add(acc[0], mm(wbuf[slot, 0], x, NT))
                add(acc[1], mm(wbuf[slot, 1], x, NT))
            if has_g:
                add(acc[0 if mode == "grad" else 2], mm(wbuf[slot, n_w - 1], do_out[0][tile], NT))
            if mode == "grad":
                add(acc[1], mm(wbuf[slot, 0], g_sc[0][tile], NT))

        @pl.when((act[i] == 1) & (c == n_c - 1))
        def _():
            if mode == "fwd":
                for copy in z_copies(i):
                    copy.start()
            else:
                if mode == "grad":
                    for copy in z_copies(i):
                        copy.wait()

                @pl.when((i != 5) & (i != 7))
                def _():
                    finish(i, tile, 0)

                finish(i, tile, 128)
                second = act[jnp.minimum(i + 1, 7)]

                @pl.when((i < 4) | (i == 5) | (i == 7) | (second == 0))
                def _():
                    for copy in hid_copies(tile):
                        copy.start()

        return 0

    lax.fori_loop(0, 8, step, 0)

    if mode == "fwd":
        @pl.when(c == n_c - 1)
        def _():
            each_active(lambda i: [copy.wait() for copy in z_copies(i)])
    else:
        @pl.when(c == n_c - 1)
        def _():
            for tile in range(6):
                for copy in hid_copies(tile):
                    copy.wait()


def experts(mode, eidx, act, slots, gates, xs, gs, weights, zs, dc, ring):
    has_x, has_g = mode != "grad", mode != "fwd"
    ff, dim = weights[0].shape[1:]
    n_c = dim // dc
    any_blk = pl.BlockSpec(memory_space=pl.ANY)
    small = pl.BlockSpec((4, 8, 256), lambda c, e, t: ORIGIN)
    v_blk = pl.BlockSpec((256, dc), lambda c, e, t: (0, c))

    outs = [(jax.ShapeDtypeStruct((6, 256, dim), BF16),
             pl.BlockSpec((6, 256, dc), lambda c, e, t: (0, 0, c)))] * (has_x + has_g)
    if mode == "fwd":
        outs += [(jax.ShapeDtypeStruct((8, ff, 256), F32), any_blk)] * 2
    hid = [((6, ff, 256), BF16)] * (3 * has_g)
    if mode == "grad":
        hid += [((6, 8, 256), F32)] + [((6, 256, ff), BF16)] * 2
    outs += [(jax.ShapeDtypeStruct(*h), any_blk) for h in hid]
    n_acc = 3 if mode == "both" else 2
    scratch = [pltpu.VMEM((8, ff, 256), F32)] * (n_acc + len(zs))
    if mode == "grad":
        scratch.append(pltpu.VMEM((6, 256, dc), BF16))
    scratch += [pltpu.VMEM((4, 384, 256), BF16), pltpu.VMEM((ring + 1, len(weights), ff, dc), BF16), pltpu.SemaphoreType.DMA((ring + 1, len(weights)))]
    if mode != "both":
        scratch.append(pltpu.SemaphoreType.DMA((2, 8)))
    if has_g:
        scratch.append(pltpu.VMEM((4, 384, 1), F32))
        scratch += [pltpu.VMEM(*h) for h in hid] + [pltpu.SemaphoreType.DMA((len(hid), 6))]
    n_v = len(xs) + len(gs)
    n_mm = 4 if mode == "both" else 2
    return pl.pallas_call(
        functools.partial(expert_kernel, mode, n_c, dc, ring),
        grid_spec=pltpu.PrefetchScalarGridSpec(
            num_scalar_prefetch=2, grid=(n_c,),
            in_specs=[small] * 2 + [v_blk] * n_v + [any_blk] * (len(weights) + len(zs)),
            out_specs=[o[1] for o in outs], scratch_shapes=scratch),
        out_shape=[o[0] for o in outs],
        compiler_params=pltpu.CompilerParams(vmem_limit_bytes=VMEM_LIMIT),
        cost_estimate=cost(n_mm * 2 * 1536 * dim * ff, 90e6),
    )(eidx, act, slots, gates, *xs, *gs, *weights, *zs)


def back_kernel(n_c, dc, ring, eidx, act, d1, d3, w1_hbm, w3_hbm, slots, o0, o1, o2, o3, r_sc, sel, wbuf, wsem):
    c = pl.program_id(0)
    outs = (o0, o1, o2, o3)

    def w_copies(f, expert, slot):
        cols = pl.ds(pl.multiple_of((f // 4) * dc, dc), dc)
        return [pltpu.make_async_copy(w.at[expert, :, cols], wbuf.at[slot, n], wsem.at[slot, n])
                for n, w in enumerate((w1_hbm, w3_hbm))]

    def ring_copies(f):
        return w_copies(f, eidx[lax.rem(f, 4)], lax.rem(f, ring))

    @pl.when(c == 0)
    def _():
        for f in range(ring - 1):
            for copy in ring_copies(jnp.int32(f)):
                copy.start()
        lane = lax.broadcasted_iota(jnp.int32, (256, 384), 1).astype(F32)
        for k in FOUR:
            hit = lane == slots[k, :, :1]
            for m in range(1, 5):
                hit = hit | (lane == slots[k, :, m:m + 1])
            sel[k] = jnp.where(hit, 1.0, 0.0).astype(BF16)

    def step(i, _):
        expert = eidx[i]
        tile = tile_of(i, eidx)
        f = c * 4 + jnp.minimum(i, 3)
        stray = (i >= 4) & (expert != eidx[3])
        slot = jnp.where(stray, ring, lax.rem(f, ring))

        @pl.when(i < 4)
        def _():
            @pl.when(f + ring - 1 < 4 * n_c)
            def _():
                for copy in ring_copies(f + ring - 1):
                    copy.start()

            for copy in ring_copies(f):
                copy.wait()

        @pl.when((act[i] == 1) & stray)
        def _():
            for copy in w_copies(f, expert, ring):
                copy.start()
            for copy in w_copies(f, expert, ring):
                copy.wait()

        @pl.when(act[i] == 1)
        def _():
            r = (mm(d1[tile], wbuf[slot, 0], NN) + mm(d3[tile], wbuf[slot, 1], NN)).astype(BF16)

            @pl.when(i < 4)
            def _():
                lo = pl.multiple_of(expert * COLD, COLD)
                for k in FOUR:
                    r_sc[k, pl.ds(lo, COLD), :] = r[COLD * k:COLD * (k + 1)]

            for q in range(2):
                @pl.when(i == 4 + 2 * q)
                def _():
                    r_sc[2 * q, 256:384, :] = r[0:128]

                @pl.when((i == 4 + 2 * q) | (i == 5 + 2 * q))
                def _():
                    r_sc[2 * q + 1, 256:384, :] = r[128:256]

        return 0

    lax.fori_loop(0, 8, step, 0)
    for k in FOUR:
        outs[k][...] = mm(sel[k], r_sc[k], NN)


def back(eidx, act, d1, d3, w1t, w3t, slots):
    ff, dim = w1t.shape[1:]
    dc, ring = 1024, 4
    n_c = dim // dc
    d_blk = pl.BlockSpec((6, 256, ff), lambda c, e, t: ORIGIN, pipeline_mode=pl.Buffered(1))
    any_blk = pl.BlockSpec(memory_space=pl.ANY)
    s_blk = pl.BlockSpec((4, 256, 8), lambda c, e, t: ORIGIN)
    return pl.pallas_call(
        functools.partial(back_kernel, n_c, dc, ring),
        grid_spec=pltpu.PrefetchScalarGridSpec(
            num_scalar_prefetch=2, grid=(n_c,),
            in_specs=[d_blk, d_blk, any_blk, any_blk, s_blk],
            out_specs=[pl.BlockSpec((256, dc), lambda c, e, t: (0, c))] * 4,
            scratch_shapes=[pltpu.VMEM((4, 384, dc), BF16), pltpu.VMEM((4, 256, 384), BF16),
                            pltpu.VMEM((ring + 1, 2, ff, dc), BF16), pltpu.SemaphoreType.DMA((ring + 1, 2))]),
        out_shape=[jax.ShapeDtypeStruct((256, dim), F32)] * 4,
        compiler_params=pltpu.CompilerParams(vmem_limit_bytes=VMEM_LIMIT),
        cost_estimate=cost(2 * 2 * 1536 * dim * ff, 70e6),
        name="back",
    )(eidx, act, d1, d3, w1t, w3t, slots)


def wgrad_kernel(info, xa, xb, ga, gb, xoa, xob, goa, gob,
                 aa, d1a, d3a, ab, d1b, d3b, w1o, w3o, w2o):
    j = pl.program_id(1)
    all_hot = info[1] == j
    for m in range(2, 9):
        all_hot = all_hot & (info[m] == j)

    def run(first, second, cols):
        def part(n, q):
            (x, g, a, d1, d3), tile = n
            return x[q, :, cols], g[q, :, cols], a[tile + q], d1[tile + q], d3[tile + q]

        def products(parts):
            w1o[0, :, cols] = sum(mm(p[3], p[0], NN) for p in parts)
            w3o[0, :, cols] = sum(mm(p[4], p[0], NN) for p in parts)
            w2o[0, :, cols] = sum(mm(p[2], p[1], NN) for p in parts)

        main = [part(first[0], 0), part(second[0], 0)]

        @pl.when(all_hot)
        def _():
            products(main + [part(n[1], q) for n in (first, second) for q in range(2)])

        @pl.when(jnp.logical_not(all_hot))
        def _():
            products(main)
            for _, over, off in (first, second):

                def body(q, _):
                    h0, h1 = info[off + 2 * q], info[off + 2 * q + 1]

                    @pl.when((h0 == j) | (h1 == j))
                    def _():
                        x, g, a, d1, d3 = part(over, q)
                        row = lax.broadcasted_iota(jnp.int32, a.shape, 1)
                        mine = jnp.where(row < 128, h0, h1) == j

                        def keep(v):
                            return jnp.where(mine, v.astype(F32), 0.0).astype(BF16)

                        w1o[0, :, cols] += mm(keep(d1), x, NN)
                        w3o[0, :, cols] += mm(keep(d3), x, NN)
                        w2o[0, :, cols] += mm(keep(a), g, NN)

                    return 0

                lax.fori_loop(0, 2, body, 0)

    na = (((xa, ga, aa, d1a, d3a), j), ((xoa, goa, aa, d1a, d3a), 4), 1)
    nb = (((xb, gb, ab, d1b, d3b), j), ((xob, gob, ab, d1b, d3b), 4), 5)

    def columns(h, _):
        cols = pl.ds(pl.multiple_of(h * 512, 512), 512)

        @pl.when(info[0] == 0)
        def _():
            run(na, nb, cols)

        @pl.when(info[0] == 1)
        def _():
            run(nb, na, cols)

        return 0

    lax.fori_loop(0, w1o.shape[2] // 512, columns, 0)


def wgrad(info, xa, ga, hid_a, xb, gb, hid_b, dim, ff):
    dc = 1024

    main_blk = pl.BlockSpec((1, 256, dc), lambda c, j, s: (j, 0, c))
    over_blk = pl.BlockSpec((2, 256, dc), lambda c, j, s: (2, 0, c))
    hid_blk = pl.BlockSpec((6, ff, 256), lambda c, j, s: ORIGIN, pipeline_mode=pl.Buffered(1))
    return pl.pallas_call(
        wgrad_kernel,
        grid_spec=pltpu.PrefetchScalarGridSpec(
            num_scalar_prefetch=1, grid=(dim // dc, 4),
            in_specs=[main_blk] * 4 + [over_blk] * 4 + [hid_blk] * 6,
            out_specs=[pl.BlockSpec((1, ff, dc), lambda c, j, s: (j, 0, c))] * 3),
        out_shape=[jax.ShapeDtypeStruct((4, ff, dim), F32)] * 3,
        compiler_params=pltpu.CompilerParams(vmem_limit_bytes=VMEM_LIMIT),
        cost_estimate=cost(3 * 2 * 3072 * dim * ff, 200e6),
        name="wgrad",
    )(info, xa, xb, ga, gb, xa, xb, ga, gb, *hid_a, *hid_b)


def solution(mesh):
    tok_spec = P(("dp", "ep"), None)
    exp_spec = P("ep", None, None)
    axes = ("dp", "ep")

    def shift(arr, dp_bit, ep_bits):
        pairs = [(s, (((s // 4) ^ dp_bit) * 4) + ((s % 4) ^ ep_bits)) for s in range(8)]
        return lax.ppermute(arr, axes, pairs)

    def device_step(x_loc, route_idx, w_router, w_gate, w_up, w_down, dy_loc):
        tok, dim = x_loc.shape
        ff = w_gate.shape[2]
        ep = lax.axis_index("ep")
        dp = lax.axis_index("dp")
        e0 = ep * 4
        w1t, w3t, w2 = jnp.swapaxes(w_gate, 1, 2), jnp.swapaxes(w_up, 1, 2), w_down

        order = jnp.arange(tok, dtype=jnp.int32)
        before = (order[:, None] < order[None, :]).astype(BF16)
        local = jnp.arange(4, dtype=jnp.int32)

        def tables(idx):
            picked = jnp.any(idx[:, None] == (e0 + local)[None, :, None, None], axis=2)
            ranks = jnp.dot(picked.reshape(16, tok).astype(BF16), before, preferred_element_type=F32)
            ranks = jnp.where(picked, ranks.reshape(4, 4, tok), -1.0)
            main = jnp.where((ranks >= 0) & (ranks < COLD), ranks + COLD * local.astype(F32)[None, :, None], -1.0)
            over = jnp.max(jnp.where(ranks >= COLD, ranks - COLD + 4 * COLD, -1.0), axis=1, keepdims=True)
            slots = jnp.concatenate([main, over, jnp.full((4, 3, tok), -1.0, F32)], axis=1)
            large = jnp.max(ranks, axis=2) >= COLD
            hot = jnp.min(jnp.where(large, local[None, :], 3), axis=1)
            first = jnp.arange(3, dtype=jnp.int32)
            first = first + (first >= hot[0])
            eidx = jnp.concatenate([first, hot[:1], hot])
            one = jnp.ones((), jnp.int32)
            act = jnp.stack([one, one, one, one, one, (hot[0] != hot[1]).astype(jnp.int32),
                             one, (hot[2] != hot[3]).astype(jnp.int32)])
            return ranks, slots, hot, eidx, act

        def gate_table(gates, ranks):
            mine = jnp.stack([lax.dynamic_slice_in_dim(v, e0, 4, axis=0) for v in gates])
            over = jnp.sum(jnp.where(ranks >= COLD, mine, 0.0), axis=1, keepdims=True)
            return jnp.concatenate([mine, over, jnp.zeros((4, 3, tok), F32)], axis=1)

        idx_t = route_idx.T
        idx_a = jnp.stack([idx_t] + [shift(idx_t, 0, k) for k in (1, 2, 3)])
        x_across = shift(x_loc, 0, 2)
        x_sib = shift(x_loc, 0, 1)
        x_y = shift(x_loc, 1, 0)
        g_across = shift(dy_loc, 0, 2)
        g_sib = shift(dy_loc, 0, 1)
        g_y = shift(dy_loc, 1, 0)
        idx_b = jnp.stack([shift(idx_t, 1, k) for k in FOUR])

        logits = jnp.dot(x_loc, w_router, preferred_element_type=F32)
        hit = route_idx[:, :, None] == jnp.arange(16, dtype=jnp.int32)
        chosen = jnp.sum(jnp.where(hit, logits[:, None, :], 0.0), axis=2)
        probs = jax.nn.softmax(chosen, axis=-1)
        gate_t = jnp.sum(jnp.where(hit, probs[:, :, None], 0.0), axis=1).T
        gates_a = [gate_t] + [shift(gate_t, 0, k) for k in (1, 2, 3)]
        gates_b = [shift(gate_t, 1, k) for k in FOUR]

        ranks_a, slots_a, hot_a, eidx_a, act_a = tables(idx_a)
        slots_t = jnp.swapaxes(slots_a, 1, 2)
        x_across_sib = shift(x_across, 0, 1)
        x_ya = shift(x_across, 1, 0)
        x_ys = shift(x_y, 0, 1)
        gate_a0 = jnp.zeros((4, 8, tok), F32)
        xa, z1_a, z3_a = experts("fwd", eidx_a, act_a, slots_a, gate_a0, (x_loc, x_sib, x_across, x_across_sib), (),
                                 (w1t, w3t), (), 2048, 3)
        z1_a, g_across, g_y = lax.optimization_barrier((z1_a, g_across, g_y))
        z3_a, gates_a, gates_b, idx_b = lax.optimization_barrier((z3_a, gates_a, gates_b, idx_b))
        ranks_b, slots_b, hot_b, eidx_b, act_b = tables(idx_b)
        g_across_sib = shift(g_across, 0, 1)
        g_ya = shift(g_across, 1, 0)
        g_ys = shift(g_y, 0, 1)
        gate_a = gate_table(gates_a, ranks_a)
        gate_b = gate_table(gates_b, ranks_b)
        da, a_a, d1_a, d3_a, q_a, d1r_a, d3r_a = experts(
            "grad", eidx_a, act_a, slots_a, gate_a, (), (dy_loc, g_sib, g_across, g_across_sib), (w2,), (z1_a, z3_a), 1024, 4)
        part = back(eidx_a, act_a, d1r_a, d3r_a, w1t, w3t, slots_t)

        q_rows = q_a[:, 0, :]
        q_main = q_rows[:4].reshape(4, 4, COLD).transpose(1, 0, 2)
        q_over = q_rows[4:].reshape(4, OVER)
        r64 = jnp.arange(COLD, dtype=F32)
        r128 = jnp.arange(OVER, dtype=F32) + COLD
        q_tok = jnp.sum(jnp.where(ranks_a[..., None] == r64, q_main[:, :, None, :], 0.0), axis=3)
        q_tok = q_tok + jnp.sum(jnp.where(ranks_a[..., None] == r128, q_over[:, None, None, :], 0.0), axis=3)
        q_recv = [shift(q_tok[k], 0, k) for k in (1, 2, 3)]

        part_own, x_ya, g_ya, q_recv = lax.optimization_barrier((part[0], x_ya, g_ya, q_recv))
        x_yas = shift(x_ya, 0, 1)
        g_yas = shift(g_ya, 0, 1)

        to_sib = shift(part[1], 0, 1)
        pair = part[2] + shift(part[3], 0, 1)

        q_back = jnp.stack([q_tok[0]] + q_recv)
        q16 = q_back[ep ^ local].reshape(16, tok)
        d_sel = gate_t * (q16 - jnp.sum(gate_t * q16, axis=0, keepdims=True))
        d_logits = d_sel.astype(BF16)
        gr = jnp.dot(d_logits, x_loc, preferred_element_type=F32)

        x_yas, g_yas, pair, gr = lax.optimization_barrier((x_yas, g_yas, pair, gr))
        from_across = shift(pair, 0, 2)
        gr = gr + shift(gr, 0, 1)
        gr_recv = shift(gr, 1, 0)
        xb, db, a_b, d1_b, d3_b = experts(
            "both", eidx_b, act_b, slots_b, gate_b, (x_y, x_ys, x_ya, x_yas), (g_y, g_ys, g_ya, g_yas),
            (w1t, w3t, w2), (), 512, 6)
        d1_b, gr_recv = lax.optimization_barrier((d1_b, gr_recv))
        gr = gr + gr_recv
        gr_recv = shift(gr, 0, 2)
        info = jnp.concatenate([dp[None].astype(jnp.int32), hot_a, hot_b])
        g1t, g3t, grad_down = wgrad(info, xa, da, (a_a, d1_a, d3_a), xb, db, (a_b, d1_b, d3_b), dim, ff)
        g1t, gr_recv, from_across, d_logits = lax.optimization_barrier((g1t, gr_recv, from_across, d_logits))
        grad_router = (gr + gr_recv).T
        du = lax.dot_general(d_logits, w_router, (((0,), (1,)), ((), ())), preferred_element_type=F32)
        grad_x = (part_own + to_sib + from_across + du).astype(BF16)
        return grad_x, jnp.swapaxes(g1t, 1, 2), jnp.swapaxes(g3t, 1, 2), grad_down, grad_router

    return jax.shard_map(device_step, mesh=mesh, in_specs=(tok_spec, tok_spec, P(), exp_spec, exp_spec, exp_spec, tok_spec), out_specs=(tok_spec, exp_spec, exp_spec, exp_spec, P()), check_vma=False)
```
